512 devices in a mesh: grp: 8 (over x, y_hi), blk: 64 (over z, y_lo, core).
Axes of the slice: x: 4, y: 8 (y_hi: 2, y_lo: 4; y = y_hi * 4 + y_lo), z: 8, core: 2. Of those that a mesh axis runs over, the one named last changes fastest.
Arguments:
- sensors: float32 [3, 131072], P(None, 'blk'), may hold values from 0 to 1
- sources: bfloat16 [3, 1048576], P(None, ('grp', 'blk')), may hold values from 0 to 1
- weights: bfloat16 [1048576], P(('grp', 'blk')), may hold values from 0.5 to 2
- probes: bfloat16 [1048576, 128], P(('grp', 'blk')), may hold values from -6 to 6
Outputs:
- response: float32 [128, 131072], P('grp', 'blk')
The draws below stay inside these ranges and needn't reach their ends.
All inputs are finite; a program needn't handle non-finite values.
Results may differ from the reference program's by a relative error of at most 0.01.
Values may be sent and summed in bfloat16 or wider, within the bound.
A program may use at most 64 MiB of HBM per device.

```python
import math
import jax
import jax.numpy as jnp
from jax import lax

SENS_DEV = 2048
SRC_DEV = 2048
PROBES = 128
STEPS = 6
SENSORS = 131072
SOURCES = 1048576
N_GRP = 8
N_BLK = 64


def block_levels(stream_key, shape, pieces, smallest, largest):
    loudness, own = 1.0, jax.random.fold_in(stream_key, 6)
    for position, shards_of in pieces:
        steps = jnp.exp(jax.random.uniform(jax.random.fold_in(own, position), (shards_of,), jnp.float32, smallest / len(pieces), largest / len(pieces)))
        loudness = loudness * jnp.repeat(steps, shape[position] // shards_of).reshape([-1 if axis == position else 1 for axis in range(len(shape))])
    return loudness


def scatter_about(rng, extent, width, limit, shards=(), kind=jnp.bfloat16):
    values = jax.random.normal(rng, extent, jnp.float32) * width
    if len(shards) > 0:
        values = block_levels(rng, extent, shards, -0.22, 0.18) * values
    return jnp.clip(values, min=-limit, max=limit).astype(kind)


def setup_inputs(seed: int = 0) -> dict:
    key_of = jax.random.split(jax.random.key(seed), 5)
    return {
        "sensors": jnp.clip(1.0 * jax.random.uniform(key_of[0], (3, SENSORS), jnp.float32) ** block_levels(key_of[0], (3, SENSORS), ((1, 64),), -0.2, 0.2), 0.0, 1.0),
        "sources": jnp.clip(1.0 * jax.random.uniform(key_of[1], (3, SOURCES), jnp.float32) ** block_levels(key_of[1], (3, SOURCES), ((1, 512),), -0.2, 0.2), 0.0, 1.0).astype(jnp.bfloat16),
        "weights": jnp.clip(jnp.exp(math.log(2.0) - 1.3862944 * jax.random.uniform(key_of[2], (SOURCES,), jnp.float32) ** block_levels(key_of[2], (SOURCES,), ((0, 512),), -0.2, 0.2)), 0.5, 2.0).astype(jnp.bfloat16),
        "probes": scatter_about(key_of[3], (SOURCES, PROBES), 1.0, 6.0, ((0, 512),)),
    }


def kernel_tile(sens, src, wgt, prb):
    dist = jnp.zeros((src.shape[1], sens.shape[1]), jnp.float32)
    for comp in range(3):
        delta = src[comp].astype(jnp.float32)[:, None] - sens[comp][None, :]
        dist = dist + delta * delta
    ker = (wgt.astype(jnp.float32)[:, None] * lax.rsqrt(dist + 0.0025)).astype(jnp.bfloat16)
    return lax.dot_general(prb, ker, (((0,), (0,)), ((), ())), preferred_element_type=jnp.float32)

def reference(sensors, sources, weights, probes):
    srcs = sources.reshape(3, N_GRP, N_BLK, SRC_DEV)
    wgts = weights.reshape(N_GRP, N_BLK, SRC_DEV)
    prbs = probes.reshape(N_GRP, N_BLK, SRC_DEV, PROBES)
    sens_all = sensors.reshape(3, N_BLK, SENS_DEV)
    scale = 1.0 / math.sqrt(STEPS * SRC_DEV * N_GRP)

    def one_block(index):
        sens = lax.dynamic_index_in_dim(sens_all, index, 1, keepdims=False)
        total = jnp.zeros((PROBES, SENS_DEV), jnp.float32)
        for group in range(N_GRP):
            part = jnp.zeros((PROBES, SENS_DEV), jnp.float32)
            for step in range(STEPS):
                other = ((index - step) % N_BLK).astype(jnp.int32)
                src = lax.dynamic_index_in_dim(srcs[:, group], other, 1, keepdims=False)
                wgt = lax.dynamic_index_in_dim(wgts[group], other, 0, keepdims=False)
                prb = lax.dynamic_index_in_dim(prbs[group], other, 0, keepdims=False)
                part = part + kernel_tile(sens, src, wgt, prb)
            rounded = lax.optimization_barrier((part * scale).astype(jnp.bfloat16))
            total = total + rounded.astype(jnp.float32)
        return total
    blocks = lax.map(one_block, jnp.arange(N_BLK, dtype=jnp.int32))
    return jnp.transpose(blocks, (1, 0, 2)).reshape(PROBES, N_BLK * SENS_DEV)
```

```python
import functools
import math

import jax
import jax.numpy as jnp
from jax import lax
from jax.experimental import pallas as pl
from jax.experimental.pallas import tpu as pltpu
from jax.sharding import PartitionSpec as P

STEPS = 6
EPS = 0.0025
BF, F32 = jnp.bfloat16, jnp.float32


def pieces(v):
    hi = v.astype(BF).astype(F32)
    mid = (v - hi).astype(BF).astype(F32)
    return [hi, mid, v - hi - mid]


def squared(v):
    return v[0:1] * v[0:1] + v[1:2] * v[1:2] + v[2:3] * v[2:3]


def kernel(
    groups, blocks, sens, src, wgt, prb, out, prb_t, lhs, rhs, ker_a, ker_b, sens_in, work, inbox, buf_a, buf_b, buf_c, buf_d, rcv,
    sens_send, sens_recv, core_send, core_recv, a_send, a_recv, b_send, b_recv, c_send, c_recv, d_send, d_recv, f_send, f_recv,
):
    sources, sensors = src.shape[1], sens.shape[1]
    half, chunk = sensors // 2, sensors // 4
    nx = groups // 2
    grp, blk = lax.axis_index("grp"), lax.axis_index("blk")
    x, yh = grp // 2, grp % 2
    core = blk % 2
    other = grp + 1 - 2 * yh
    at = lambda offset: (blk + offset + blocks) % blocks
    x_next = ((x + 1) % nx) * 2 + yh
    x_prev = ((x + nx - 1) % nx) * 2 + yh
    peer = blk + 1 - 2 * core

    barrier = pltpu.get_barrier_semaphore()
    near = [(grp, at(o)) for o in range(-STEPS + 1, STEPS) if o != 0]
    near += [(other, at(o)) for o in range(-STEPS + 1, STEPS)]
    near += [(x_next, blk), (x_prev, blk)]
    for device in near:
        pl.semaphore_signal(barrier, inc=1, device_id=device, device_id_type=pl.DeviceIdType.MESH)

    def copy(source, target, send, recv, device):
        return pltpu.make_async_remote_copy(source, target, send, recv, device_id=device, device_id_type=pl.DeviceIdType.MESH)

    started = []

    def send(*args):
        started.append(copy(*args))
        started[-1].start()

    scale = 1.0 / math.sqrt(STEPS * sources * groups)
    prb_t[...] = (jnp.transpose(prb[...].astype(F32)) * (wgt[...].astype(F32) * scale)).astype(BF)
    place = src[...].astype(F32)
    ones = jnp.ones((1, sources), F32)
    rows = [-2.0 * place] * 3 + [ones] * 3 + pieces(squared(place)) + [jnp.zeros((113, sources), F32)]
    lhs[...] = jnp.transpose(jnp.concatenate(rows, axis=0)).astype(BF)
    rhs[...] = jnp.zeros_like(rhs)
    sens_in[0] = sens[...]

    def offset_of(step):
        if step == 0:
            return 0
        if step == 1:
            return jnp.where(core == 0, 1, STEPS - 1)
        return 7 - step - core

    def piece_of(step, j):
        if step < 2:
            alone = core == step
            return jnp.where(alone, j, 3 - j)
        return 2 * step + 1 - j

    def prepare(step, j):
        columns = jnp.where(core == j, half, 0)
        where = sens_in[offset_of(step), :, pl.ds(pl.multiple_of(columns, 128), half)]
        parts = pieces(where)
        ones_row = jnp.ones((3, half), F32)
        rows = parts + pieces(squared(where) + EPS) + [ones_row, jnp.zeros((1, half), F32)]
        rhs[j, 0:16] = jnp.concatenate(rows, axis=0).astype(BF)

    def distances(n):
        ker = (ker_a, ker_b)[n % 2]
        dist = jnp.dot(lhs[...], rhs[(n % 4) // 2, :, pl.ds((n % 2) * chunk, chunk)], preferred_element_type=F32)
        ker[...] = lax.rsqrt(dist).astype(BF)

    def apply(n):
        ker = (ker_a, ker_b)[n % 2]
        part = jnp.dot(prb_t[...], ker[...], preferred_element_type=F32)
        part = part.astype(BF).reshape(groups, part.shape[0] // groups, chunk)
        work[piece_of(n // 4, (n % 4) // 2), :, :, pl.ds((n % 2) * chunk, chunk)] = part

    def unit_kk(u):
        return 6 * core if u < 2 else (1, 5, 4, 3, 2)[u - 2]

    def unit_at(u):
        return u if u < 2 else 2 * u - 2

    def unit_half(u):
        return core if u > 0 else 1 - core

    far, fore, back = (x + 2) % nx * 2, (x + 1) % nx * 2, (x + nx - 1) % nx * 2

    def stage1(u):
        w = unit_at(u)
        if u >= 2:
            s = u - 2
            copy(work.at[w], inbox.at[s], core_send.at[s], core_recv.at[s], (grp, peer)).wait_recv()
            work[w] = (work[w].astype(F32) + inbox[s].astype(F32)).astype(BF)
        send(work.at[w, far], buf_a.at[u], a_send.at[u], a_recv.at[u], (x_next, blk))
        send(work.at[w, far + 1], buf_b.at[u], b_send.at[u], b_recv.at[u], (x_prev, blk))

    def stage2(u):
        w = unit_at(u)
        copy(buf_a.at[u], buf_a.at[u], a_send.at[u], a_recv.at[u], (x_prev, blk)).wait_recv()
        work[w, fore] = (work[w, fore].astype(F32) + buf_a[u].astype(F32)).astype(BF)
        send(work.at[w, pl.ds(fore, 2)], buf_c.at[u], c_send.at[u], c_recv.at[u], (x_next, blk))
        copy(buf_b.at[u], buf_b.at[u], b_send.at[u], b_recv.at[u], (x_next, blk)).wait_recv()
        work[w, back + 1] = (work[w, back + 1].astype(F32) + buf_b[u].astype(F32)).astype(BF)
        send(work.at[w, pl.ds(back, 2)], buf_d.at[u], d_send.at[u], d_recv.at[u], (x_prev, blk))

    def final(u, away):
        w, kk, h = unit_at(u), unit_kk(u), unit_half(u)
        row = grp if away == 0 else other
        device = (row, at(kk - core))
        return copy(work.at[w, row], rcv.at[kk // 2, away, h], f_send.at[u, away], f_recv.at[kk // 2, away, h], device)

    def stage3(u):
        w, kk, h = unit_at(u), unit_kk(u), unit_half(u)
        copy(buf_c.at[u], buf_c.at[u], c_send.at[u], c_recv.at[u], (x_prev, blk)).wait_recv()
        copy(buf_d.at[u], buf_d.at[u], d_send.at[u], d_recv.at[u], (x_next, blk)).wait_recv()
        own = pl.ds(x * 2, 2)
        work[w, own] = (work[w, own].astype(F32) + buf_c[u].astype(F32) + buf_d[u].astype(F32)).astype(BF)
        final(u, 1).start()
        if u < 3:
            mine = core == (0 if u < 2 else 1)

            @pl.when(mine)
            def _():
                rcv[0, 0, h] = work[w, grp]

            @pl.when(jnp.logical_not(mine))
            def _():
                final(u, 0).start()
        else:
            final(u, 0).start()

    def finish_final(u):
        final(u, 1).wait_send()
        if u < 3:

            @pl.when(core != (0 if u < 2 else 1))
            def _():
                final(u, 0).wait_send()
        else:
            final(u, 0).wait_send()

    batches = {1: (0, 1, 2), 2: (3,), 3: (4,), 4: (5,), 5: (6,)}
    total = 4 * STEPS
    prepare(0, 0)
    distances(0)
    for n in range(total):
        step, j, last = n // 4, (n % 4) // 2, n % 2 == 1
        if n == 1:
            pl.semaphore_wait(barrier, len(near))
            for o in range(1, STEPS):
                send(sens, sens_in.at[o], sens_send.at[o - 1], sens_recv.at[o - 1], (grp, at(-o)))
        if n + 1 < total:
            if n + 1 == 4:
                for o in range(1, STEPS):
                    copy(sens, sens_in.at[o], sens_send.at[o - 1], sens_recv.at[o - 1], (grp, at(o))).wait_recv()
            if (n + 1) % 2 == 0:
                prepare((n + 1) // 4, ((n + 1) % 4) // 2)
            distances(n + 1)
        apply(n)
        if last and step >= 1:
            if j == 0:
                s = step - 1
                send(work.at[3 + 2 * s], inbox.at[s], core_send.at[s], core_recv.at[s], (grp, peer))
            else:
                for u in batches[step]:
                    stage1(u)
                for u in batches.get(step - 1, ()):
                    stage2(u)
                for u in batches.get(step - 2, ()):
                    stage3(u)
    stage2(6)
    stage3(5)
    stage3(6)

    sums = [None, None]
    for q in range(3):
        for away in range(2):
            for h in range(2):
                slot = rcv.at[q, away, h]

                def wait(slot=slot, index=(q, away, h)):
                    copy(slot, slot, f_send.at[0, 0], f_recv.at[index], (other, blk)).wait_recv()

                if q > 0 or away > 0:
                    wait()
                elif h == 0:
                    pl.when(core == 1)(wait)
    for h in range(2):
        for q in range(3):
            for away in range(2):
                term = rcv[q, away, h].astype(F32)
                sums[h] = term if sums[h] is None else sums[h] + term
        out[:, h * half : (h + 1) * half] = sums[h]

    @pl.when(core == 0)
    def _():
        for h in range(2):
            for away in range(2):
                copy(rcv.at[3, away, h], rcv.at[3, away, h], f_send.at[0, 0], f_recv.at[3, away, h], (other, blk)).wait_recv()
            out[:, h * half : (h + 1) * half] = sums[h] + (rcv[3, 0, h].astype(F32) + rcv[3, 1, h].astype(F32))

    for sent in started:
        sent.wait_send()
    for u in range(7):
        finish_final(u)


def solution(mesh):
    groups, blocks = mesh.shape["grp"], mesh.shape["blk"]

    def step(sensors, sources, weights, probes):
        (columns, probe), count = (sensors.shape[1], probes.shape[1]), probes.shape[0]
        rows, half, chunk = probe // groups, columns // 2, columns // 4
        vmem = pl.BlockSpec(memory_space=pltpu.VMEM)
        dma = pltpu.SemaphoreType.DMA
        return pl.pallas_call(
            functools.partial(kernel, groups, blocks),
            out_shape=jax.ShapeDtypeStruct((rows, columns), F32),
            in_specs=[vmem] * 4,
            out_specs=vmem,
            scratch_shapes=[
                pltpu.VMEM((probe, count), BF),
                pltpu.VMEM((count, 128), BF),
                pltpu.VMEM((2, 128, half), BF),
                pltpu.VMEM((count, chunk), BF),
                pltpu.VMEM((count, chunk), BF),
                pltpu.VMEM((STEPS, 3, columns), F32),
                pltpu.VMEM((12, groups, rows, half), BF),
                pltpu.VMEM((5, groups, rows, half), BF),
                pltpu.VMEM((7, rows, half), BF),
                pltpu.VMEM((7, rows, half), BF),
                pltpu.VMEM((7, 2, rows, half), BF),
                pltpu.VMEM((7, 2, rows, half), BF),
                pltpu.VMEM((4, 2, 2, rows, half), BF),
            ]
            + [dma((n,)) for n in (5, 5, 5, 5, 7, 7, 7, 7, 7, 7, 7, 7)]
            + [dma((7, 2)), dma((4, 2, 2))],
            compiler_params=pltpu.CompilerParams(collective_id=0, has_side_effects=True, vmem_limit_bytes=48 * 2**20),
        )(sensors, sources, weights.reshape(1, -1), probes)

    in_specs = (P(None, "blk"), P(None, ("grp", "blk")), P(("grp", "blk")), P(("grp", "blk"), None))
    return jax.shard_map(step, mesh=mesh, in_specs=in_specs, out_specs=P("grp", "blk"), check_vma=False)
```

```python
import functools
import math

import jax
import jax.numpy as jnp
from jax import lax
from jax.experimental import pallas as pl
from jax.experimental.pallas import tpu as pltpu
from jax.sharding import PartitionSpec as P

STEPS = 6
EPS = 0.0025
BF, F32 = jnp.bfloat16, jnp.float32
MESH = pl.DeviceIdType.MESH

ORDER = ((0, 0, 5, 5, 4, 4, 3, 3, 2, 2, 1, 1), (1, 1, 6, 6, 5, 5, 4, 4, 3, 3, 2, 2))
TILE = 256
ON_MXU = 256


def pieces(v):
    hi = v.astype(BF).astype(F32)
    mid = (v - hi).astype(BF).astype(F32)
    return [hi, mid, v - hi - mid]


def squared(v):
    return v[0:1] * v[0:1] + v[1:2] * v[1:2] + v[2:3] * v[2:3]


def kernel(
    groups, blocks, sens, src, wgt, prb, out, prb_in, src_in, wgt_in, prb_t, lhs, lanes, rhs, rows_of, ker_a, ker_b, sens_in, work,
    inbox, buf_a, buf_b, buf_c, buf_d, rcv, load, ready, sens_send, sens_recv, core_send, core_recv, a_send, a_recv, b_send, b_recv,
    c_send, c_recv, d_send, d_recv, f_send, f_recv,
):
    sources, sensors = src.shape[1], sens.shape[1]
    half, chunk = sensors // 2, sensors // 4
    nx = groups // 2
    grp, blk = lax.axis_index("grp"), lax.axis_index("blk")
    x, yh = grp // 2, grp % 2
    core = blk % 2
    other = grp + 1 - 2 * yh
    x_next = ((x + 1) % nx) * 2 + yh
    x_prev = ((x + nx - 1) % nx) * 2 + yh
    peer = blk + 1 - 2 * core

    def at(offset):
        return (blk + offset + blocks) % blocks

    def by_core(a, b):
        return a if a == b else jnp.where(core == 0, a, b)

    def signal(semaphore, device):
        pl.semaphore_signal(semaphore, inc=1, device_id=device, device_id_type=MESH)

    def copy(source, target, send, recv, device):
        return pltpu.make_async_remote_copy(source, target, send, recv, device_id=device, device_id_type=MESH)

    started = []

    def send(*args):
        started.append(copy(*args))
        started[-1].start()

    barrier = pltpu.get_barrier_semaphore()
    for o in range(1, STEPS):
        signal(barrier, (grp, at(-o)))
        pl.when(blk + o < blocks)(lambda o=o: signal(barrier, (grp, at(o))))
    for o in range(STEPS):
        signal(barrier, (other, at(-o)))
    for row in (x_next, x_prev):
        signal(barrier, (row, blk))
    expected = 3 * STEPS - jnp.maximum(STEPS - 1 - blk, 0)

    loads = [
        pltpu.make_async_copy(ref, target, load.at[i])
        for i, (ref, target) in enumerate(((src, src_in), (sens, sens_in.at[0]), (wgt, wgt_in), (prb, prb_in)))
    ]
    for step in loads:
        step.start()
    rhs[...] = jnp.zeros_like(rhs)

    loads[0].wait()
    place = src_in[...].astype(F32)
    rows = [-2.0 * place] * 3 + [jnp.ones((3, sources), F32)] + pieces(squared(place)) + [jnp.zeros((113, sources), F32)]
    lhs[...] = jnp.transpose(jnp.concatenate(rows, axis=0)).astype(BF)
    if ON_MXU < chunk:
        for i in range(3):
            lanes[i] = jnp.transpose(jnp.broadcast_to(place[i : i + 1], (128, sources))).astype(BF)
    loads[1].wait()
    loads[2].wait()
    scale = 1.0 / math.sqrt(STEPS * sources * groups)
    weight = wgt_in[...].astype(F32) * scale
    weight = jnp.concatenate([weight[i : i + 1] for i in range(weight.shape[0])], axis=1)
    loads[3].wait()
    prb_t[...] = (jnp.transpose(prb_in[...].astype(F32)) * weight).astype(BF)

    def turn(hs):
        return by_core(ORDER[0][hs], ORDER[1][hs]), hs % 2

    def slot_of(hs):
        kk0, kk1 = ORDER[0][hs], ORDER[1][hs]
        j = hs % 2
        return by_core(j if kk0 == 0 else 2 * kk0 + 1 - j, j if kk1 == 6 else 2 * kk1 + 1 - j)

    def prepare(hs):
        kk, j = turn(hs)
        columns = jnp.where(core == j, half, 0)
        where = sens_in[kk - core, :, pl.ds(pl.multiple_of(columns, 128), half)]
        parts = pieces(where)
        rows = parts + pieces(squared(where) + EPS) + [jnp.ones((3, half), F32), jnp.zeros((1, half), F32)]
        rhs[hs % 2, 0:16] = jnp.concatenate(rows, axis=0).astype(BF)
        rows_of[hs % 2] = jnp.concatenate([parts[0], where - parts[0], jnp.zeros((2, half), F32)], axis=0)

    def evaluate(n, k):
        ker, hs, first = (ker_a, ker_b)[n % 2], n // 2, (n % 2) * chunk
        span = pl.ds(k * TILE, TILE)
        dist = jnp.dot(lhs[span], rhs[hs % 2, :, pl.ds(first, ON_MXU)], preferred_element_type=F32)
        ker[span, 0:ON_MXU] = lax.rsqrt(dist).astype(BF)
        width = chunk - ON_MXU
        if width == 0:
            return
        near = [
            jnp.broadcast_to(rows_of[hs % 2, i : i + 1, pl.ds(first + ON_MXU, width)], (16, width)).astype(BF) for i in range(6)
        ]
        for r in range(k * TILE, (k + 1) * TILE, 16):
            total = None
            for i in range(3):
                delta = jnp.concatenate([lanes[i, r : r + 16]] * (width // 128), axis=1) - near[i] - near[3 + i]
                total = delta * delta if total is None else total + delta * delta
            ker[r : r + 16, ON_MXU:chunk] = lax.rsqrt(total + jnp.asarray(EPS, BF))

    def block(n):
        part = None
        for k in range(sources // TILE):
            if n + 1 < 4 * STEPS:
                evaluate(n + 1, k)
            if n >= 0:
                span = pl.ds(k * TILE, TILE)
                term = jnp.dot(prb_t[:, span], (ker_a, ker_b)[n % 2][span], preferred_element_type=F32)
                part = term if part is None else part + term
        if n >= 0:
            part = part.astype(BF).reshape(groups, part.shape[0] // groups, chunk)
            work[slot_of(n // 2), :, :, pl.ds((n % 2) * chunk, chunk)] = part

    def unit_kk(u):
        return by_core(*((0, 6), (0, 6), (5, 5), (4, 4), (3, 3), (2, 1), (1, 2))[u])

    def unit_at(u):
        return u if u < 2 else 2 * unit_kk(u)

    def unit_half(u):
        return core if u > 0 else 1 - core

    far, fore, back = (x + 2) % nx * 2, (x + 1) % nx * 2, (x + nx - 1) % nx * 2

    def to_peer(kk):
        return copy(work.at[2 * kk + 1], inbox.at[kk - 1], core_send.at[kk - 1], core_recv.at[kk - 1], (grp, peer))

    def stage1(u):
        w = unit_at(u)
        if u >= 2:
            kk = unit_kk(u)
            to_peer(kk).wait_recv()
            work[w] = (work[w].astype(F32) + inbox[kk - 1].astype(F32)).astype(BF)
        send(work.at[w, far], buf_a.at[u], a_send.at[u], a_recv.at[u], (x_next, blk))
        send(work.at[w, far + 1], buf_b.at[u], b_send.at[u], b_recv.at[u], (x_prev, blk))

    def stage2(u):
        w = unit_at(u)
        copy(buf_a.at[u], buf_a.at[u], a_send.at[u], a_recv.at[u], (x_prev, blk)).wait_recv()
        work[w, fore] = (work[w, fore].astype(F32) + buf_a[u].astype(F32)).astype(BF)
        send(work.at[w, pl.ds(fore, 2)], buf_c.at[u], c_send.at[u], c_recv.at[u], (x_next, blk))
        copy(buf_b.at[u], buf_b.at[u], b_send.at[u], b_recv.at[u], (x_next, blk)).wait_recv()
        work[w, back + 1] = (work[w, back + 1].astype(F32) + buf_b[u].astype(F32)).astype(BF)
        send(work.at[w, pl.ds(back, 2)], buf_d.at[u], d_send.at[u], d_recv.at[u], (x_prev, blk))

    def final(u, away):
        w, kk, h = unit_at(u), unit_kk(u), unit_half(u)
        row = grp if away == 0 else other
        device = (row, at(kk - core))
        return copy(work.at[w, row], rcv.at[kk // 2, away, h], f_send.at[u, away], f_recv.at[kk // 2, away, h], device)

    holder = {0: 0, 1: 0, 5: 1}

    def stage3(u):
        w, h = unit_at(u), unit_half(u)
        copy(buf_c.at[u], buf_c.at[u], c_send.at[u], c_recv.at[u], (x_prev, blk)).wait_recv()
        copy(buf_d.at[u], buf_d.at[u], d_send.at[u], d_recv.at[u], (x_next, blk)).wait_recv()
        own = pl.ds(x * 2, 2)
        work[w, own] = (work[w, own].astype(F32) + buf_c[u].astype(F32) + buf_d[u].astype(F32)).astype(BF)
        final(u, 1).start()
        if u in holder:

            @pl.when(core == holder[u])
            def _():
                rcv[0, 0, h] = work[w, grp]

            @pl.when(core != holder[u])
            def _():
                final(u, 0).start()
        else:
            final(u, 0).start()

    def sensors_to(o):
        copy(sens_in.at[0], sens_in.at[o], sens_send.at[o - 1], sens_recv.at[o - 1], (grp, at(-o))).start()

    def sensors_late(o):
        pl.semaphore_wait(ready.at[o - 1], 1)
        sensors_to(o)

    def meet():
        with jax.named_scope("barrier_wait"):
            pl.semaphore_wait(barrier, expected)
        for o in range(1, STEPS):
            pl.when(blk + o >= blocks)(lambda o=o: signal(ready.at[o - 1], (grp, at(o))))
            pl.when(blk >= o)(lambda o=o: sensors_to(o))

    def scoped(name, action, *args):
        with jax.named_scope(name):
            action(*args)

    def late():
        for o in range(1, STEPS):
            pl.when(blk < o)(functools.partial(sensors_late, o))

    def arrived():
        for o in range(1, STEPS):
            copy(sens_in.at[0], sens_in.at[o], sens_send.at[o - 1], sens_recv.at[o - 1], (grp, at(o))).wait_recv()

    def peer_send(kk0, kk1):
        if kk0 is None:
            pl.when(core == 1)(lambda: to_peer(kk1).start())
        elif kk1 is None:
            pl.when(core == 0)(lambda: to_peer(kk0).start())
        else:
            to_peer(by_core(kk0, kk1)).start()

    s1, s2, s3 = ((f"s{i + 1}", f) for i, f in enumerate((stage1, stage2, stage3)))
    after = {
        0: [("meet", meet)],
        1: [("core", peer_send, None, 1)],
        5: [("core", peer_send, 5, None)],
        7: [(*s1, 0), (*s1, 1)],
        9: [("core", peer_send, 4, 5)],
        11: [(*s1, 2), (*s2, 0), (*s2, 1)],
        13: [("core", peer_send, 3, 4)],
        15: [(*s1, 3), (*s2, 2), (*s3, 0), (*s3, 1)],
        17: [("core", peer_send, 2, 3)],
        19: [(*s1, 4), (*s2, 3), (*s3, 2)],
        21: [("core", peer_send, 1, 2), (*s3, 3)],
        22: [(*s1, 5), (*s2, 4)],
        23: [(*s1, 6), (*s2, 5), (*s2, 6), (*s3, 4), (*s3, 5), (*s3, 6)],
    }
    after.setdefault(9, []).append(("late", late))
    prepare(0)
    block(-1)
    for n in range(4 * STEPS):
        if n == 3:
            scoped("sens_wait", arrived)
        if n % 2 == 1 and n + 1 < 4 * STEPS:
            prepare((n + 1) // 2)
        block(n)
        for name, action, *args in after.get(n, ()):
            scoped("_".join([name, *map(str, args)]), action, *args)

    def landed(q, away, h):
        slot = rcv.at[q, away, h]
        copy(slot, slot, f_send.at[0, 0], f_recv.at[q, away, h], (other, blk)).wait_recv()

    def total(slots, h, base=None):
        for q, away in slots:
            term = rcv[q, away, h].astype(F32)
            base = term if base is None else base + term
        return base

    def gather():
        for h in range(2):
            pl.when(core == 0)(lambda h=h: [landed(3, 0, h), landed(3, 1, h)][0])
            for q in (2, 1):
                for away in range(2):
                    landed(q, away, h)
        pl.when(core == 1)(lambda: landed(0, 0, 0))
        for h in range(2):
            landed(0, 1, h)

    scoped("gather", gather)
    for h in range(2):
        part = total([(q, away) for q in range(3) for away in range(2)], h)
        far_part = total([(3, 0), (3, 1)], h)
        out[:, h * half : (h + 1) * half] = jnp.where(core == 0, part + far_part, part)

    for o in range(1, STEPS):
        copy(sens_in.at[0], sens_in.at[o], sens_send.at[o - 1], sens_recv.at[o - 1], (grp, at(-o))).wait_send()
    for kk in range(1, STEPS):
        to_peer(kk).wait_send()
    for sent in started:
        sent.wait_send()
    for u in range(7):
        final(u, 1).wait_send()
        if u in holder:
            pl.when(core != holder[u])(lambda u=u: final(u, 0).wait_send())
        else:
            final(u, 0).wait_send()


def solution(mesh):
    groups, blocks = mesh.shape["grp"], mesh.shape["blk"]

    def step(sensors, sources, weights, probes):
        (columns, probe), count = (sensors.shape[1], probes.shape[1]), probes.shape[0]
        rows, half, chunk = probe // groups, columns // 2, columns // 4
        dma = pltpu.SemaphoreType.DMA
        return pl.pallas_call(
            functools.partial(kernel, groups, blocks),
            out_shape=jax.ShapeDtypeStruct((rows, columns), F32),
            in_specs=[pl.BlockSpec(memory_space=pl.ANY)] * 4,
            out_specs=pl.BlockSpec(memory_space=pltpu.VMEM),
            scratch_shapes=[
                pltpu.VMEM((count, probe), BF),
                pltpu.VMEM((3, count), BF),
                pltpu.VMEM((count // 128, 128), BF),
                pltpu.VMEM((probe, count), BF),
                pltpu.VMEM((count, 128), BF),
                pltpu.VMEM((3, count, 128), BF),
                pltpu.VMEM((2, 128, half), BF),
                pltpu.VMEM((2, 8, half), F32),
                pltpu.VMEM((count, chunk), BF),
                pltpu.VMEM((count, chunk), BF),
                pltpu.VMEM((STEPS, 3, columns), F32),
                pltpu.VMEM((12, groups, rows, half), BF),
                pltpu.VMEM((5, groups, rows, half), BF),
                pltpu.VMEM((7, rows, half), BF),
                pltpu.VMEM((7, rows, half), BF),
                pltpu.VMEM((7, 2, rows, half), BF),
                pltpu.VMEM((7, 2, rows, half), BF),
                pltpu.VMEM((4, 2, 2, rows, half), BF),
                dma((4,)),
                pltpu.SemaphoreType.REGULAR((5,)),
            ]
            + [dma((n,)) for n in (5, 5, 5, 5, 7, 7, 7, 7, 7, 7, 7, 7)]
            + [dma((7, 2)), dma((4, 2, 2))],
            compiler_params=pltpu.CompilerParams(collective_id=0, has_side_effects=True, vmem_limit_bytes=63 * 2**20),
        )(sensors, sources, weights.reshape(-1, 128), probes)

    in_specs = (P(None, "blk"), P(None, ("grp", "blk")), P(("grp", "blk")), P(("grp", "blk"), None))
    return jax.shard_map(step, mesh=mesh, in_specs=in_specs, out_specs=P("grp", "blk"), check_vma=False)
```

```python
import functools
import math

import jax
import jax.numpy as jnp
from jax import lax
from jax.experimental import pallas as pl
from jax.experimental.pallas import tpu as pltpu
from jax.sharding import PartitionSpec as P

STEPS = 6
EPS = 0.0025
BF, F32 = jnp.bfloat16, jnp.float32
MESH = pl.DeviceIdType.MESH

ORDER = ((0, 0, 1, 1, 2, 2, 5, 5, 4, 4, 3, 3), (1, 1, 2, 2, 6, 6, 5, 5, 4, 4, 3, 3))
TILE = 256
ON_MXU = 512


def pieces(v):
    hi = v.astype(BF).astype(F32)
    mid = (v - hi).astype(BF).astype(F32)
    return [hi, mid, v - hi - mid]


def squared(v):
    return v[0:1] * v[0:1] + v[1:2] * v[1:2] + v[2:3] * v[2:3]


def kernel(
    groups, blocks, sens, src, wgt, prb, out, own_sens, prb_in, src_in, wgt_in, prb_t, lhs, lanes, rhs, rows_of, ker_a, ker_b, sens_in, work,
    inbox, buf_a, buf_b, buf_c, buf_d, rcv, load, ready, sens_send, sens_recv, core_send, core_recv, a_send, a_recv, b_send, b_recv,
    c_send, c_recv, d_send, d_recv, f_send, f_recv,
):
    sources, sensors = src.shape[1], sens.shape[1]
    half, chunk = sensors // 2, sensors // 4
    nx = groups // 2
    grp, blk = lax.axis_index("grp"), lax.axis_index("blk")
    x, yh = grp // 2, grp % 2
    core = blk % 2
    other = grp + 1 - 2 * yh
    x_next = ((x + 1) % nx) * 2 + yh
    x_prev = ((x + nx - 1) % nx) * 2 + yh
    peer = blk + 1 - 2 * core

    def at(offset):
        return (blk + offset + blocks) % blocks

    def by_core(a, b):
        return a if a == b else jnp.where(core == 0, a, b)

    def signal(semaphore, device):
        pl.semaphore_signal(semaphore, inc=1, device_id=device, device_id_type=MESH)

    def copy(source, target, send, recv, device):
        return pltpu.make_async_remote_copy(source, target, send, recv, device_id=device, device_id_type=MESH)

    started = []

    def send(*args):
        started.append(copy(*args))
        started[-1].start()

    barrier = pltpu.get_barrier_semaphore()
    for o in range(1, STEPS):
        signal(barrier, (grp, at(-o)))
        pl.when(blk + o < blocks)(lambda o=o: signal(barrier, (grp, at(o))))
    for o in range(STEPS):
        signal(barrier, (other, at(-o)))
    for row in (x_next, x_prev):
        signal(barrier, (row, blk))
    expected = 3 * STEPS - jnp.maximum(STEPS - 1 - blk, 0)

    loads = [
        pltpu.make_async_copy(ref, target, load.at[i])
        for i, (ref, target) in enumerate(((src, src_in), (sens, own_sens), (wgt, wgt_in), (prb, prb_in)))
    ]
    for step in loads:
        step.start()
    rhs[...] = jnp.zeros_like(rhs)

    @pl.when(blk > blocks - STEPS)
    def _():
        pl.semaphore_wait(barrier, expected)
        for o in range(1, STEPS):
            pl.when(blk + o >= blocks)(lambda o=o: signal(ready.at[o - 1], (grp, at(o))))

    loads[0].wait()
    place = src_in[...].astype(F32)
    rows = [-2.0 * place] * 3 + [jnp.ones((3, sources), F32)] + pieces(squared(place)) + [jnp.zeros((113, sources), F32)]
    lhs[...] = jnp.transpose(jnp.concatenate(rows, axis=0)).astype(BF)
    if ON_MXU < chunk:
        for i in range(3):
            lanes[i] = jnp.transpose(jnp.broadcast_to(place[i : i + 1], (128, sources))).astype(BF)
    loads[1].wait()
    width = sensors // 8
    for r in range(8):
        span = slice(r * width, (r + 1) * width)
        sens_in[0, r : r + 1] = jnp.concatenate([own_sens[i : i + 1, span] for i in range(3)], axis=1)
    loads[2].wait()
    scale = 1.0 / math.sqrt(STEPS * sources * groups)
    weight = wgt_in[...].astype(F32) * scale
    weight = jnp.concatenate([weight[i : i + 1] for i in range(weight.shape[0])], axis=1)
    loads[3].wait()
    prb_t[...] = (jnp.transpose(prb_in[...]).astype(F32) * weight).astype(BF)

    def turn(hs):
        return by_core(ORDER[0][hs], ORDER[1][hs]), hs % 2

    def slot_of(hs):
        kk0, kk1 = ORDER[0][hs], ORDER[1][hs]
        j = hs % 2
        return by_core(j if kk0 == 0 else 2 * kk0 + 1 - j, j if kk1 == 6 else 2 * kk1 + 1 - j)

    def prepare(hs):
        kk, j = turn(hs)
        packed = sens_in[kk - core]
        packed = jnp.where(core == j, packed[4:8], packed[0:4])
        where = jnp.concatenate(
            [jnp.concatenate([packed[r : r + 1, i * width : (i + 1) * width] for r in range(4)], axis=1) for i in range(3)], axis=0
        )
        parts = pieces(where)
        rows = parts + pieces(squared(where) + EPS) + [jnp.ones((3, half), F32), jnp.zeros((1, half), F32)]
        rhs[hs % 2, 0:16] = jnp.concatenate(rows, axis=0).astype(BF)
        rows_of[hs % 2] = jnp.concatenate([parts[0], where - parts[0], jnp.zeros((2, half), F32)], axis=0)

    def evaluate(n, k):
        ker, hs, first = (ker_a, ker_b)[n % 2], n // 2, (n % 2) * chunk
        span = pl.ds(k * TILE, TILE)
        dist = jnp.dot(lhs[span], rhs[hs % 2, :, pl.ds(first, ON_MXU)], preferred_element_type=F32)
        ker[span, 0:ON_MXU] = lax.rsqrt(dist).astype(BF)
        width = chunk - ON_MXU
        if width == 0:
            return
        near = [
            jnp.broadcast_to(rows_of[hs % 2, i : i + 1, pl.ds(first + ON_MXU, width)], (16, width)).astype(BF) for i in range(6)
        ]
        for r in range(k * TILE, (k + 1) * TILE, 16):
            total = None
            for i in range(3):
                delta = jnp.concatenate([lanes[i, r : r + 16]] * (width // 128), axis=1) - near[i] - near[3 + i]
                total = delta * delta if total is None else total + delta * delta
            ker[r : r + 16, ON_MXU:chunk] = lax.rsqrt(total + jnp.asarray(EPS, BF))

    def block(n):
        part = None
        for k in range(sources // TILE):
            if n + 1 < 4 * STEPS:
                evaluate(n + 1, k)
            if n >= 0:
                span = pl.ds(k * TILE, TILE)
                term = jnp.dot(prb_t[:, span], (ker_a, ker_b)[n % 2][span], preferred_element_type=F32)
                part = term if part is None else part + term
        if n >= 0:
            part = part.astype(BF).reshape(groups, part.shape[0] // groups, chunk)
            work[slot_of(n // 2), n % 2] = part

    def unit_kk(u):
        return 6 * core if u < 2 else (1, 2, 5, 4, 3)[u - 2]

    def unit_at(u):
        return u if u < 2 else 2 * unit_kk(u)

    def unit_half(u):
        return core if u > 0 else 1 - core

    far, fore, back = (x + 2) % nx * 2, (x + 1) % nx * 2, (x + nx - 1) % nx * 2

    def to_peer(kk, c):
        s = kk - 1
        return copy(work.at[2 * kk + 1, c], inbox.at[s, c], core_send.at[s, c], core_recv.at[s, c], (grp, peer))

    def stage1(u, c):
        w = unit_at(u)
        if u >= 2:
            kk = unit_kk(u)
            to_peer(kk, c).wait_recv()
            work[w, c] = (work[w, c].astype(F32) + inbox[kk - 1, c].astype(F32)).astype(BF)
        send(work.at[w, c, far], buf_a.at[u, c], a_send.at[u, c], a_recv.at[u, c], (x_next, blk))
        send(work.at[w, c, far + 1], buf_b.at[u, c], b_send.at[u, c], b_recv.at[u, c], (x_prev, blk))

    def stage2(u, c):
        w = unit_at(u)
        copy(buf_a.at[u, c], buf_a.at[u, c], a_send.at[u, c], a_recv.at[u, c], (x_prev, blk)).wait_recv()
        work[w, c, fore] = (work[w, c, fore].astype(F32) + buf_a[u, c].astype(F32)).astype(BF)
        send(work.at[w, c, pl.ds(fore, 2)], buf_c.at[u, c], c_send.at[u, c], c_recv.at[u, c], (x_next, blk))
        copy(buf_b.at[u, c], buf_b.at[u, c], b_send.at[u, c], b_recv.at[u, c], (x_next, blk)).wait_recv()
        work[w, c, back + 1] = (work[w, c, back + 1].astype(F32) + buf_b[u, c].astype(F32)).astype(BF)
        send(work.at[w, c, pl.ds(back, 2)], buf_d.at[u, c], d_send.at[u, c], d_recv.at[u, c], (x_prev, blk))

    def final(u, c, away):
        w, kk, h = unit_at(u), unit_kk(u), unit_half(u)
        row = grp if away == 0 else other
        q = kk // 2
        return copy(work.at[w, c, row], rcv.at[q, away, h, c], f_send.at[u, c, away], f_recv.at[q, away, h, c], (row, at(kk - core)))

    holder = {0: 0, 1: 0, 2: 1}

    def stage3(u, c):
        w, h = unit_at(u), unit_half(u)
        copy(buf_c.at[u, c], buf_c.at[u, c], c_send.at[u, c], c_recv.at[u, c], (x_prev, blk)).wait_recv()
        copy(buf_d.at[u, c], buf_d.at[u, c], d_send.at[u, c], d_recv.at[u, c], (x_next, blk)).wait_recv()
        own = pl.ds(x * 2, 2)
        work[w, c, own] = (work[w, c, own].astype(F32) + buf_c[u, c].astype(F32) + buf_d[u, c].astype(F32)).astype(BF)
        final(u, c, 1).start()
        if u in holder:

            @pl.when(core == holder[u])
            def _():
                rcv[0, 0, h, c] = work[w, c, grp]

            @pl.when(core != holder[u])
            def _():
                final(u, c, 0).start()
        else:
            final(u, c, 0).start()

    def sensors_to(o):
        copy(sens_in.at[0], sens_in.at[o], sens_send.at[o - 1], sens_recv.at[o - 1], (grp, at(-o))).start()

    def sensors_late(o):
        pl.semaphore_wait(ready.at[o - 1], 1)
        sensors_to(o)

    def meet():
        with jax.named_scope("barrier_wait"):
            pl.when(blk <= blocks - STEPS)(lambda: pl.semaphore_wait(barrier, expected))
        for o in range(1, STEPS):
            pl.when(blk >= o)(lambda o=o: sensors_to(o))

    def scoped(name, action, *args):
        with jax.named_scope(name):
            action(*args)

    def late():
        for o in range(1, STEPS):
            pl.when(blk < o)(functools.partial(sensors_late, o))

    def arrived():
        for o in range(1, STEPS):
            copy(sens_in.at[0], sens_in.at[o], sens_send.at[o - 1], sens_recv.at[o - 1], (grp, at(o))).wait_recv()

    s1, s2, s3, both = "s1", "s2", "s3", (0, 1)
    does = {
        s1: stage1, s2: stage2, s3: stage3, "core": lambda kk, c: to_peer(kk, c).start(), "meet": meet, "late": late,
    }
    pair = lambda name, *units: [(name, u, c) for u in units for c in both]
    after = {
        0: [("meet",)],
        5: pair("core", 1),
        8: pair(s1, 2),
        9: pair("core", 2),
        11: pair(s1, 0, 1),
        12: pair(s1, 3) + pair(s2, 2),
        13: pair("core", 5),
        15: pair(s1, 4) + pair(s2, 0),
        16: pair(s2, 1, 3) + pair(s3, 2),
        17: pair("core", 4),
        19: pair(s1, 5) + pair(s2, 4) + pair(s3, 0),
        20: [("core", 3, 0)] + pair(s3, 1, 3),
        21: [("core", 3, 1)],
        22: [(s1, 6, 0)] + pair(s2, 5),
        23: [(s1, 6, 1)] + pair(s3, 4) + pair(s2, 6) + pair(s3, 5, 6),
    }
    after.setdefault(9, []).append(("late",))
    prepare(0)
    block(-1)
    for n in range(4 * STEPS):
        if n == 3:
            scoped("sens_wait", arrived)
        if n % 2 == 1 and n + 1 < 4 * STEPS:
            prepare((n + 1) // 2)
        block(n)
        for name, *args in after.get(n, ()):
            scoped("_".join([name, *map(str, args)]), does[name], *args)

    def landed(q, away, h):
        for c in both:
            slot = rcv.at[q, away, h, c]
            copy(slot, slot, f_send.at[0, 0, 0], f_recv.at[q, away, h, c], (other, blk)).wait_recv()

    def total(slots, h, c):
        base = None
        for q, away in slots:
            term = rcv[q, away, h, c].astype(F32)
            base = term if base is None else base + term
        return base

    def gather():
        pl.when(core == 1)(lambda: landed(0, 0, 0))
        for h in both:
            landed(0, 1, h)
            landed(2, 0, h)
            landed(2, 1, h)

            @pl.when(core == 0)
            def _(h=h):
                landed(3, 0, h)
                landed(3, 1, h)

            landed(1, 0, h)
            landed(1, 1, h)

    scoped("gather", gather)
    for h in both:
        for c in both:
            part = total([(q, away) for q in range(3) for away in both], h, c)
            far_part = total([(3, 0), (3, 1)], h, c)
            first = h * half + c * chunk
            out[:, first : first + chunk] = jnp.where(core == 0, part + far_part, part)

    for o in range(1, STEPS):
        copy(sens_in.at[0], sens_in.at[o], sens_send.at[o - 1], sens_recv.at[o - 1], (grp, at(-o))).wait_send()
    for kk in range(1, STEPS):
        for c in both:
            to_peer(kk, c).wait_send()
    for sent in started:
        sent.wait_send()
    for u in range(7):
        for c in both:
            final(u, c, 1).wait_send()
            if u in holder:
                pl.when(core != holder[u])(lambda u=u, c=c: final(u, c, 0).wait_send())
            else:
                final(u, c, 0).wait_send()


def solution(mesh):
    groups, blocks = mesh.shape["grp"], mesh.shape["blk"]

    def step(sensors, sources, weights, probes):
        (columns, probe), count = (sensors.shape[1], probes.shape[1]), probes.shape[0]
        rows, half, chunk = probe // groups, columns // 2, columns // 4
        dma = pltpu.SemaphoreType.DMA
        return pl.pallas_call(
            functools.partial(kernel, groups, blocks),
            out_shape=jax.ShapeDtypeStruct((rows, columns), F32),
            in_specs=[pl.BlockSpec(memory_space=pl.ANY)] * 4,
            out_specs=pl.BlockSpec(memory_space=pltpu.VMEM),
            scratch_shapes=[
                pltpu.VMEM((3, columns), F32),
                pltpu.VMEM((count, probe), BF),
                pltpu.VMEM((3, count), BF),
                pltpu.VMEM((count // 128, 128), BF),
                pltpu.VMEM((probe, count), BF),
                pltpu.VMEM((count, 128), BF),
                pltpu.VMEM((3, count if ON_MXU < chunk else 16, 128), BF),
                pltpu.VMEM((2, 128, half), BF),
                pltpu.VMEM((2, 8, half), F32),
                pltpu.VMEM((count, chunk), BF),
                pltpu.VMEM((count, chunk), BF),
                pltpu.VMEM((STEPS, 8, 3 * columns // 8), F32),
                pltpu.VMEM((12, 2, groups, rows, chunk), BF),
                pltpu.VMEM((5, 2, groups, rows, chunk), BF),
                pltpu.VMEM((7, 2, rows, chunk), BF),
                pltpu.VMEM((7, 2, rows, chunk), BF),
                pltpu.VMEM((7, 2, 2, rows, chunk), BF),
                pltpu.VMEM((7, 2, 2, rows, chunk), BF),
                pltpu.VMEM((4, 2, 2, 2, rows, chunk), BF),
                dma((4,)),
                pltpu.SemaphoreType.REGULAR((5,)),
                dma((5,)),
                dma((5,)),
                dma((5, 2)),
                dma((5, 2)),
            ]
            + [dma((7, 2))] * 8
            + [dma((7, 2, 2)), dma((4, 2, 2, 2))],
            compiler_params=pltpu.CompilerParams(collective_id=0, has_side_effects=True, vmem_limit_bytes=48 * 2**20),
        )(sensors, sources, weights.reshape(-1, 128), probes)

    in_specs = (P(None, "blk"), P(None, ("grp", "blk")), P(("grp", "blk")), P(("grp", "blk"), None))
    return jax.shard_map(step, mesh=mesh, in_specs=in_specs, out_specs=P("grp", "blk"), check_vma=False)
```

```python
import functools
import math

import jax
import jax.numpy as jnp
from jax import lax
from jax.experimental import pallas as pl
from jax.experimental.pallas import tpu as pltpu
from jax.sharding import PartitionSpec as P

STEPS = 6
EPS = 0.0025
BF, F32 = jnp.bfloat16, jnp.float32
MESH = pl.DeviceIdType.MESH

ORDER = ((0, 0, 1, 1, 2, 2, 5, 5, 4, 4, 3, 3), (1, 1, 2, 2, 6, 6, 5, 5, 4, 4, 3, 3))
NEEDED = (1, 2, 5, 4, 3)
TILE = 256
ON_MXU = 512


def pieces(v):
    hi = v.astype(BF).astype(F32)
    mid = (v - hi).astype(BF).astype(F32)
    return [hi, mid, v - hi - mid]


def squared(v):
    return v[0:1] * v[0:1] + v[1:2] * v[1:2] + v[2:3] * v[2:3]


def kernel(
    groups, blocks, sens, src, wgt, prb, out, own_sens, prb_in, src_in, wgt_in, prb_t, lhs, lanes, rhs, rows_of, ker_a, ker_b, sens_in, work,
    inbox, buf_a, buf_b, buf_c, buf_d, rcv, load, ready, sens_send, sens_recv, core_send, core_recv, a_send, a_recv, b_send, b_recv,
    c_send, c_recv, d_send, d_recv, f_send, f_recv,
):
    sources, sensors = src.shape[1], sens.shape[1]
    half, chunk = sensors // 2, sensors // 4
    nx = groups // 2
    grp, blk = lax.axis_index("grp"), lax.axis_index("blk")
    x, yh = grp // 2, grp % 2
    core = blk % 2
    other = grp + 1 - 2 * yh
    x_next = ((x + 1) % nx) * 2 + yh
    x_prev = ((x + nx - 1) % nx) * 2 + yh
    peer = blk + 1 - 2 * core

    def at(offset):
        return (blk + offset + blocks) % blocks

    def by_core(a, b):
        return a if a == b else jnp.where(core == 0, a, b)

    def signal(semaphore, device):
        pl.semaphore_signal(semaphore, inc=1, device_id=device, device_id_type=MESH)

    def copy(source, target, send, recv, device):
        return pltpu.make_async_remote_copy(source, target, send, recv, device_id=device, device_id_type=MESH)

    started = []

    def send(*args):
        started.append(copy(*args))
        started[-1].start()

    barrier = pltpu.get_barrier_semaphore()
    for o in range(1, STEPS):
        signal(barrier, (grp, at(-o)))
        pl.when(blk + o < blocks)(lambda o=o: signal(barrier, (grp, at(o))))
    for o in range(STEPS):
        signal(barrier, (other, at(-o)))
    for row in (x_next, x_prev):
        signal(barrier, (row, blk))
    expected = 3 * STEPS - jnp.maximum(STEPS - 1 - blk, 0)

    loads = [
        pltpu.make_async_copy(ref, target, load.at[i])
        for i, (ref, target) in enumerate(((src, src_in), (sens, own_sens), (wgt, wgt_in), (prb, prb_in)))
    ]
    for step in loads:
        step.start()
    rhs[...] = jnp.zeros_like(rhs)

    @pl.when(blk > blocks - STEPS)
    def _():
        pl.semaphore_wait(barrier, expected)
        for o in range(1, STEPS):
            pl.when(blk + o >= blocks)(lambda o=o: signal(ready.at[o - 1], (grp, at(o))))

    loads[0].wait()
    place = src_in[...].astype(F32)
    rows = [-2.0 * place] * 3 + [jnp.ones((3, sources), F32)] + pieces(squared(place)) + [jnp.zeros((113, sources), F32)]
    lhs[...] = jnp.transpose(jnp.concatenate(rows, axis=0)).astype(BF)
    if ON_MXU < chunk:
        for i in range(3):
            lanes[i] = jnp.transpose(jnp.broadcast_to(place[i : i + 1], (128, sources))).astype(BF)
    loads[1].wait()
    width = sensors // 8
    for r in range(8):
        span = slice(r * width, (r + 1) * width)
        sens_in[0, r : r + 1] = jnp.concatenate([own_sens[i : i + 1, span] for i in range(3)], axis=1)
    loads[2].wait()
    scale = 1.0 / math.sqrt(STEPS * sources * groups)
    weight = wgt_in[...].astype(F32) * scale
    weight = jnp.concatenate([weight[i : i + 1] for i in range(weight.shape[0])], axis=1)
    loads[3].wait()
    prb_t[...] = (jnp.transpose(prb_in[...]).astype(F32) * weight).astype(BF)

    def turn(hs):
        return by_core(ORDER[0][hs], ORDER[1][hs]), hs % 2

    def slot_of(hs):
        kk0, kk1 = ORDER[0][hs], ORDER[1][hs]
        j = hs % 2
        return by_core(j if kk0 == 0 else 2 * kk0 + 1 - j, j if kk1 == 6 else 2 * kk1 + 1 - j)

    def prepare(hs):
        kk, j = turn(hs)
        packed = sens_in[kk - core]
        packed = jnp.where(core == j, packed[4:8], packed[0:4])
        where = jnp.concatenate(
            [jnp.concatenate([packed[r : r + 1, i * width : (i + 1) * width] for r in range(4)], axis=1) for i in range(3)], axis=0
        )
        parts = pieces(where)
        rows = parts + pieces(squared(where) + EPS) + [jnp.ones((3, half), F32), jnp.zeros((1, half), F32)]
        rhs[hs % 2, 0:16] = jnp.concatenate(rows, axis=0).astype(BF)
        rows_of[hs % 2] = jnp.concatenate([parts[0], where - parts[0], jnp.zeros((2, half), F32)], axis=0)

    def evaluate(n, k):
        ker, hs, first = (ker_a, ker_b)[n % 2], n // 2, (n % 2) * chunk
        span = pl.ds(k * TILE, TILE)
        dist = jnp.dot(lhs[span], rhs[hs % 2, :, pl.ds(first, ON_MXU)], preferred_element_type=F32)
        ker[span, 0:ON_MXU] = lax.rsqrt(dist).astype(BF)
        width = chunk - ON_MXU
        if width == 0:
            return
        near = [
            jnp.broadcast_to(rows_of[hs % 2, i : i + 1, pl.ds(first + ON_MXU, width)], (16, width)).astype(BF) for i in range(6)
        ]
        for r in range(k * TILE, (k + 1) * TILE, 16):
            total = None
            for i in range(3):
                delta = jnp.concatenate([lanes[i, r : r + 16]] * (width // 128), axis=1) - near[i] - near[3 + i]
                total = delta * delta if total is None else total + delta * delta
            ker[r : r + 16, ON_MXU:chunk] = lax.rsqrt(total + jnp.asarray(EPS, BF))

    def block(n):
        part = None
        for k in range(sources // TILE):
            if n + 1 < 4 * STEPS:
                evaluate(n + 1, k)
            if n >= 0:
                span = pl.ds(k * TILE, TILE)
                term = jnp.dot(prb_t[:, span], (ker_a, ker_b)[n % 2][span], preferred_element_type=F32)
                part = term if part is None else part + term
        if n >= 0:
            part = part.astype(BF).reshape(groups, part.shape[0] // groups, chunk)
            work[slot_of(n // 2), n % 2] = part

    def unit_kk(u):
        return 6 * core if u < 2 else (1, 2, 5, 4, 3)[u - 2]

    def unit_at(u):
        return u if u < 2 else 2 * unit_kk(u)

    def unit_half(u):
        return core if u > 0 else 1 - core

    far, fore, back = (x + 2) % nx * 2, (x + 1) % nx * 2, (x + nx - 1) % nx * 2

    def to_peer(kk, c):
        s = kk - 1
        return copy(work.at[2 * kk + 1, c], inbox.at[s, c], core_send.at[s, c], core_recv.at[s, c], (grp, peer))

    def stage1(u, c):
        w = unit_at(u)
        if u >= 2:
            kk = unit_kk(u)
            to_peer(kk, c).wait_recv()
            work[w, c] = (work[w, c].astype(F32) + inbox[kk - 1, c].astype(F32)).astype(BF)
        send(work.at[w, c, far], buf_a.at[u, c], a_send.at[u, c], a_recv.at[u, c], (x_next, blk))
        send(work.at[w, c, far + 1], buf_b.at[u, c], b_send.at[u, c], b_recv.at[u, c], (x_prev, blk))

    def stage2(u, c):
        w = unit_at(u)
        copy(buf_a.at[u, c], buf_a.at[u, c], a_send.at[u, c], a_recv.at[u, c], (x_prev, blk)).wait_recv()
        work[w, c, fore] = (work[w, c, fore].astype(F32) + buf_a[u, c].astype(F32)).astype(BF)
        send(work.at[w, c, pl.ds(fore, 2)], buf_c.at[u, c], c_send.at[u, c], c_recv.at[u, c], (x_next, blk))
        copy(buf_b.at[u, c], buf_b.at[u, c], b_send.at[u, c], b_recv.at[u, c], (x_next, blk)).wait_recv()
        work[w, c, back + 1] = (work[w, c, back + 1].astype(F32) + buf_b[u, c].astype(F32)).astype(BF)
        send(work.at[w, c, pl.ds(back, 2)], buf_d.at[u, c], d_send.at[u, c], d_recv.at[u, c], (x_prev, blk))

    def final(u, c, away):
        w, kk, h = unit_at(u), unit_kk(u), unit_half(u)
        row = grp if away == 0 else other
        q = kk // 2
        return copy(work.at[w, c, row], rcv.at[q, away, h, c], f_send.at[u, c, away], f_recv.at[q, away, h, c], (row, at(kk - core)))

    holder = {0: 0, 1: 0, 2: 1}

    def stage3(u, c):
        w, h = unit_at(u), unit_half(u)
        copy(buf_c.at[u, c], buf_c.at[u, c], c_send.at[u, c], c_recv.at[u, c], (x_prev, blk)).wait_recv()
        copy(buf_d.at[u, c], buf_d.at[u, c], d_send.at[u, c], d_recv.at[u, c], (x_next, blk)).wait_recv()
        own = pl.ds(x * 2, 2)
        work[w, c, own] = (work[w, c, own].astype(F32) + buf_c[u, c].astype(F32) + buf_d[u, c].astype(F32)).astype(BF)
        final(u, c, 1).start()
        if u in holder:

            @pl.when(core == holder[u])
            def _():
                rcv[0, 0, h, c] = work[w, c, grp]

            @pl.when(core != holder[u])
            def _():
                final(u, c, 0).start()
        else:
            final(u, c, 0).start()

    def sensors_to(o):
        copy(sens_in.at[0], sens_in.at[o], sens_send.at[o - 1], sens_recv.at[o - 1], (grp, at(-o))).start()

    def sensors_late(o):
        pl.semaphore_wait(ready.at[o - 1], 1)
        sensors_to(o)

    def meet():
        with jax.named_scope("barrier_wait"):
            pl.when(blk <= blocks - STEPS)(lambda: pl.semaphore_wait(barrier, expected))
        for o in NEEDED:
            pl.when(blk >= o)(lambda o=o: sensors_to(o))

    def scoped(name, action, *args):
        with jax.named_scope(name):
            action(*args)

    def late():
        for o in NEEDED:
            pl.when(blk < o)(functools.partial(sensors_late, o))

    def arrived(hs):
        t = turn(hs)[0] - core
        copy(sens_in.at[0], sens_in.at[t], sens_send.at[t - 1], sens_recv.at[t - 1], (grp, at(t))).wait_recv()

    s1, s2, s3, both = "s1", "s2", "s3", (0, 1)
    does = {
        s1: stage1, s2: stage2, s3: stage3, "core": lambda kk, c: to_peer(kk, c).start(), "meet": meet, "late": late,
    }
    pair = lambda name, *units: [(name, u, c) for u in units for c in both]
    after = {
        0: [("meet",)],
        5: pair("core", 1),
        8: pair(s1, 2),
        9: pair("core", 2),
        11: pair(s1, 0, 1),
        12: pair(s1, 3) + pair(s2, 2),
        13: pair("core", 5),
        15: pair(s1, 4) + pair(s2, 0),
        16: pair(s2, 1, 3) + pair(s3, 2),
        17: pair("core", 4),
        19: pair(s1, 5) + pair(s2, 4) + pair(s3, 0),
        20: [("core", 3, 0)] + pair(s3, 1, 3),
        21: [("core", 3, 1)],
        22: [(s1, 6, 0)] + pair(s2, 5),
        23: [(s1, 6, 1)] + pair(s3, 4) + pair(s2, 6) + pair(s3, 5, 6),
    }
    after.setdefault(8, []).append(("late",))
    prepare(0)
    block(-1)
    for n in range(4 * STEPS):
        if n % 2 == 1 and n + 1 < 4 * STEPS:
            if n % 4 == 3:
                scoped(f"sens_wait_{n}", arrived, (n + 1) // 2)
            prepare((n + 1) // 2)
        block(n)
        for name, *args in after.get(n, ()):
            scoped("_".join([name, *map(str, args)]), does[name], *args)

    def landed(q, away, h):
        for c in both:
            slot = rcv.at[q, away, h, c]
            copy(slot, slot, f_send.at[0, 0, 0], f_recv.at[q, away, h, c], (other, blk)).wait_recv()

    def total(slots, h, c):
        base = None
        for q, away in slots:
            term = rcv[q, away, h, c].astype(F32)
            base = term if base is None else base + term
        return base

    def gather():
        pl.when(core == 1)(lambda: landed(0, 0, 0))
        for h in both:
            landed(0, 1, h)
            landed(2, 0, h)
            landed(2, 1, h)

            @pl.when(core == 0)
            def _(h=h):
                landed(3, 0, h)
                landed(3, 1, h)

            landed(1, 0, h)
            landed(1, 1, h)

    scoped("gather", gather)
    for h in both:
        for c in both:
            part = total([(q, away) for q in range(3) for away in both], h, c)
            far_part = total([(3, 0), (3, 1)], h, c)
            first = h * half + c * chunk
            out[:, first : first + chunk] = jnp.where(core == 0, part + far_part, part)

    for o in range(1, STEPS):
        copy(sens_in.at[0], sens_in.at[o], sens_send.at[o - 1], sens_recv.at[o - 1], (grp, at(-o))).wait_send()
    for kk in range(1, STEPS):
        for c in both:
            to_peer(kk, c).wait_send()
    for sent in started:
        sent.wait_send()
    for u in range(7):
        for c in both:
            final(u, c, 1).wait_send()
            if u in holder:
                pl.when(core != holder[u])(lambda u=u, c=c: final(u, c, 0).wait_send())
            else:
                final(u, c, 0).wait_send()


def solution(mesh):
    groups, blocks = mesh.shape["grp"], mesh.shape["blk"]

    def step(sensors, sources, weights, probes):
        (columns, probe), count = (sensors.shape[1], probes.shape[1]), probes.shape[0]
        rows, half, chunk = probe // groups, columns // 2, columns // 4
        dma = pltpu.SemaphoreType.DMA
        return pl.pallas_call(
            functools.partial(kernel, groups, blocks),
            out_shape=jax.ShapeDtypeStruct((rows, columns), F32),
            in_specs=[pl.BlockSpec(memory_space=pltpu.HBM)] * 4,
            out_specs=pl.BlockSpec(memory_space=pltpu.VMEM),
            scratch_shapes=[
                pltpu.VMEM((3, columns), F32),
                pltpu.VMEM((count, probe), BF),
                pltpu.VMEM((3, count), BF),
                pltpu.VMEM((count // 128, 128), BF),
                pltpu.VMEM((probe, count), BF),
                pltpu.VMEM((count, 128), BF),
                pltpu.VMEM((3, count if ON_MXU < chunk else 16, 128), BF),
                pltpu.VMEM((2, 128, half), BF),
                pltpu.VMEM((2, 8, half), F32),
                pltpu.VMEM((count, chunk), BF),
                pltpu.VMEM((count, chunk), BF),
                pltpu.VMEM((STEPS, 8, 3 * columns // 8), F32),
                pltpu.VMEM((12, 2, groups, rows, chunk), BF),
                pltpu.VMEM((5, 2, groups, rows, chunk), BF),
                pltpu.VMEM((7, 2, rows, chunk), BF),
                pltpu.VMEM((7, 2, rows, chunk), BF),
                pltpu.VMEM((7, 2, 2, rows, chunk), BF),
                pltpu.VMEM((7, 2, 2, rows, chunk), BF),
                pltpu.VMEM((4, 2, 2, 2, rows, chunk), BF),
                dma((4,)),
                pltpu.SemaphoreType.REGULAR((5,)),
                dma((5,)),
                dma((5,)),
                dma((5, 2)),
                dma((5, 2)),
            ]
            + [dma((7, 2))] * 8
            + [dma((7, 2, 2)), dma((4, 2, 2, 2))],
            compiler_params=pltpu.CompilerParams(collective_id=0, has_side_effects=True, vmem_limit_bytes=48 * 2**20),
        )(sensors, sources, weights.reshape(-1, 128), probes)

    in_specs = (P(None, "blk"), P(None, ("grp", "blk")), P(("grp", "blk")), P(("grp", "blk"), None))
    return jax.shard_map(step, mesh=mesh, in_specs=in_specs, out_specs=P("grp", "blk"), check_vma=False)
```

```python
import functools
import math

import jax
import jax.numpy as jnp
from jax import lax
from jax.experimental import pallas as pl
from jax.experimental.pallas import tpu as pltpu
from jax.sharding import PartitionSpec as P

STEPS = 6
EPS = 0.0025
BF, F32 = jnp.bfloat16, jnp.float32
MESH = pl.DeviceIdType.MESH

ORDER = ((0, 0, 1, 1, 2, 2, 5, 5, 4, 4, 3, 3), (1, 1, 2, 2, 6, 6, 5, 5, 4, 4, 3, 3))
NEEDED = (1, 2, 5, 4, 3)
TILE = 256
ON_MXU = 256


def pieces(v):
    hi = v.astype(BF).astype(F32)
    mid = (v - hi).astype(BF).astype(F32)
    return [hi, mid, v - hi - mid]


def squared(v):
    return v[0:1] * v[0:1] + v[1:2] * v[1:2] + v[2:3] * v[2:3]


def kernel(
    groups, blocks, sens, src, wgt, prb, out, own_sens, prb_in, src_in, wgt_in, prb_t, lhs, lanes, rhs, rows_of, ker_a, ker_b, sens_in, work,
    inbox, buf_a, buf_b, buf_c, buf_d, rcv, load, ready, sens_send, sens_recv, core_send, core_recv, a_send, a_recv, b_send, b_recv,
    c_send, c_recv, d_send, d_recv, f_send, f_recv,
):
    sources, sensors = src.shape[1], sens.shape[1]
    half, chunk = sensors // 2, sensors // 4
    nx = groups // 2
    grp, blk = lax.axis_index("grp"), lax.axis_index("blk")
    x, yh = grp // 2, grp % 2
    core = blk % 2
    other = grp + 1 - 2 * yh
    x_next = ((x + 1) % nx) * 2 + yh
    x_prev = ((x + nx - 1) % nx) * 2 + yh
    peer = blk + 1 - 2 * core

    def at(offset):
        return (blk + offset + blocks) % blocks

    def by_core(a, b):
        return a if a == b else jnp.where(core == 0, a, b)

    def signal(semaphore, device):
        pl.semaphore_signal(semaphore, inc=1, device_id=device, device_id_type=MESH)

    def copy(source, target, send, recv, device):
        return pltpu.make_async_remote_copy(source, target, send, recv, device_id=device, device_id_type=MESH)

    started = []

    def send(*args):
        started.append(copy(*args))
        started[-1].start()

    barrier = pltpu.get_barrier_semaphore()
    for o in range(1, STEPS):
        signal(barrier, (grp, at(-o)))
        pl.when(blk + o < blocks)(lambda o=o: signal(barrier, (grp, at(o))))
    for o in range(STEPS):
        signal(barrier, (other, at(-o)))
    for row in (x_next, x_prev):
        signal(barrier, (row, blk))
    expected = 3 * STEPS - jnp.maximum(STEPS - 1 - blk, 0)

    loads = [
        pltpu.make_async_copy(ref, target, load.at[i])
        for i, (ref, target) in enumerate(((src, src_in), (sens, own_sens), (wgt, wgt_in), (prb, prb_in)))
    ]
    for step in loads:
        step.start()
    rhs[...] = jnp.zeros_like(rhs)

    @pl.when(blk > blocks - STEPS)
    def _():
        pl.semaphore_wait(barrier, expected)
        for o in range(1, STEPS):
            pl.when(blk + o >= blocks)(lambda o=o: signal(ready.at[o - 1], (grp, at(o))))

    loads[0].wait()
    place = src_in[...].astype(F32)
    rows = [-2.0 * place] * 3 + [jnp.ones((3, sources), F32)] + pieces(squared(place)) + [jnp.zeros((113, sources), F32)]
    lhs[...] = jnp.transpose(jnp.concatenate(rows, axis=0)).astype(BF)
    if ON_MXU < chunk:
        row, column = (lax.broadcasted_iota(jnp.int32, (128, 384), d) for d in range(2))
        spread = jnp.where(row == column // 128, -0.5, 0.0).astype(BF)
        copies = jnp.dot(lhs[...], spread, preferred_element_type=F32).astype(BF)
        for i in range(3):
            lanes[i] = copies[:, i * 128 : (i + 1) * 128]
    loads[1].wait()
    width = sensors // 8
    for r in range(8):
        span = slice(r * width, (r + 1) * width)
        sens_in[0, r : r + 1] = jnp.concatenate([own_sens[i : i + 1, span] for i in range(3)], axis=1)
    loads[2].wait()
    scale = 1.0 / math.sqrt(STEPS * sources * groups)
    weight = wgt_in[...].astype(F32) * scale
    weight = jnp.concatenate([weight[i : i + 1] for i in range(weight.shape[0])], axis=1)
    loads[3].wait()
    prb_t[...] = (jnp.transpose(prb_in[...]).astype(F32) * weight).astype(BF)

    def turn(hs):
        return by_core(ORDER[0][hs], ORDER[1][hs]), hs % 2

    def slot_of(hs):
        kk0, kk1 = ORDER[0][hs], ORDER[1][hs]
        j = hs % 2
        return by_core(j if kk0 == 0 else 2 * kk0 + 1 - j, j if kk1 == 6 else 2 * kk1 + 1 - j)

    def prepare(hs):
        kk, j = turn(hs)
        packed = sens_in[kk - core]
        packed = jnp.where(core == j, packed[4:8], packed[0:4])
        where = jnp.concatenate(
            [jnp.concatenate([packed[r : r + 1, i * width : (i + 1) * width] for r in range(4)], axis=1) for i in range(3)], axis=0
        )
        parts = pieces(where)
        rows = parts + pieces(squared(where) + EPS) + [jnp.ones((3, half), F32), jnp.zeros((1, half), F32)]
        rhs[hs % 2, 0:16] = jnp.concatenate(rows, axis=0).astype(BF)
        rows_of[hs % 2] = jnp.concatenate([parts[0], where - parts[0], jnp.zeros((2, half), F32)], axis=0)

    def evaluate(n, k):
        ker, hs, first = (ker_a, ker_b)[n % 2], n // 2, (n % 2) * chunk
        span = pl.ds(k * TILE, TILE)
        dist = jnp.dot(lhs[span], rhs[hs % 2, :, pl.ds(first, ON_MXU)], preferred_element_type=F32)
        ker[span, 0:ON_MXU] = lax.rsqrt(dist).astype(BF)
        width = chunk - ON_MXU
        if width == 0:
            return
        near = [
            jnp.broadcast_to(rows_of[hs % 2, i : i + 1, pl.ds(first + ON_MXU, width)], (16, width)).astype(BF) for i in range(6)
        ]
        for r in range(k * TILE, (k + 1) * TILE, 16):
            total = None
            for i in range(3):
                delta = jnp.concatenate([lanes[i, r : r + 16]] * (width // 128), axis=1) - near[i] - near[3 + i]
                total = delta * delta if total is None else total + delta * delta
            ker[r : r + 16, ON_MXU:chunk] = lax.rsqrt(total + jnp.asarray(EPS, BF))

    def block(n):
        part = None
        for k in range(sources // TILE):
            if n + 1 < 4 * STEPS:
                evaluate(n + 1, k)
            if n >= 0:
                span = pl.ds(k * TILE, TILE)
                term = jnp.dot(prb_t[:, span], (ker_a, ker_b)[n % 2][span], preferred_element_type=F32)
                part = term if part is None else part + term
        if n >= 0:
            part = part.astype(BF).reshape(groups, part.shape[0] // groups, chunk)
            work[slot_of(n // 2), n % 2] = part

    def unit_kk(u):
        return 6 * core if u < 2 else (1, 2, 5, 4, 3)[u - 2]

    def unit_at(u):
        return u if u < 2 else 2 * unit_kk(u)

    def unit_half(u):
        return core if u > 0 else 1 - core

    far, fore, back = (x + 2) % nx * 2, (x + 1) % nx * 2, (x + nx - 1) % nx * 2

    def to_peer(kk, c):
        s = kk - 1
        return copy(work.at[2 * kk + 1, c], inbox.at[s, c], core_send.at[s, c], core_recv.at[s, c], (grp, peer))

    def stage1(u, c):
        w = unit_at(u)
        if u >= 2:
            kk = unit_kk(u)
            to_peer(kk, c).wait_recv()
            work[w, c] = (work[w, c].astype(F32) + inbox[kk - 1, c].astype(F32)).astype(BF)
        send(work.at[w, c, far], buf_a.at[u, c], a_send.at[u, c], a_recv.at[u, c], (x_next, blk))
        send(work.at[w, c, far + 1], buf_b.at[u, c], b_send.at[u, c], b_recv.at[u, c], (x_prev, blk))

    def stage2(u, c):
        w = unit_at(u)
        copy(buf_a.at[u, c], buf_a.at[u, c], a_send.at[u, c], a_recv.at[u, c], (x_prev, blk)).wait_recv()
        work[w, c, fore] = (work[w, c, fore].astype(F32) + buf_a[u, c].astype(F32)).astype(BF)
        send(work.at[w, c, pl.ds(fore, 2)], buf_c.at[u, c], c_send.at[u, c], c_recv.at[u, c], (x_next, blk))
        copy(buf_b.at[u, c], buf_b.at[u, c], b_send.at[u, c], b_recv.at[u, c], (x_next, blk)).wait_recv()
        work[w, c, back + 1] = (work[w, c, back + 1].astype(F32) + buf_b[u, c].astype(F32)).astype(BF)
        send(work.at[w, c, pl.ds(back, 2)], buf_d.at[u, c], d_send.at[u, c], d_recv.at[u, c], (x_prev, blk))

    def final(u, c, away):
        w, kk, h = unit_at(u), unit_kk(u), unit_half(u)
        row = grp if away == 0 else other
        q = kk // 2
        return copy(work.at[w, c, row], rcv.at[q, away, h, c], f_send.at[u, c, away], f_recv.at[q, away, h, c], (row, at(kk - core)))

    holder = {0: 0, 1: 0, 2: 1}

    def stage3(u, c):
        w, h = unit_at(u), unit_half(u)
        copy(buf_c.at[u, c], buf_c.at[u, c], c_send.at[u, c], c_recv.at[u, c], (x_prev, blk)).wait_recv()
        copy(buf_d.at[u, c], buf_d.at[u, c], d_send.at[u, c], d_recv.at[u, c], (x_next, blk)).wait_recv()
        own = pl.ds(x * 2, 2)
        work[w, c, own] = (work[w, c, own].astype(F32) + buf_c[u, c].astype(F32) + buf_d[u, c].astype(F32)).astype(BF)
        final(u, c, 1).start()
        if u in holder:

            @pl.when(core == holder[u])
            def _():
                rcv[0, 0, h, c] = work[w, c, grp]

            @pl.when(core != holder[u])
            def _():
                final(u, c, 0).start()
        else:
            final(u, c, 0).start()

    def sensors_to(o):
        copy(sens_in.at[0], sens_in.at[o], sens_send.at[o - 1], sens_recv.at[o - 1], (grp, at(-o))).start()

    def sensors_late(o):
        pl.semaphore_wait(ready.at[o - 1], 1)
        sensors_to(o)

    def meet():
        with jax.named_scope("barrier_wait"):
            pl.when(blk <= blocks - STEPS)(lambda: pl.semaphore_wait(barrier, expected))
        for o in NEEDED:
            pl.when(blk >= o)(lambda o=o: sensors_to(o))

    def scoped(name, action, *args):
        with jax.named_scope(name):
            action(*args)

    def late():
        for o in NEEDED:
            pl.when(blk < o)(functools.partial(sensors_late, o))

    def arrived(hs):
        t = turn(hs)[0] - core
        copy(sens_in.at[0], sens_in.at[t], sens_send.at[t - 1], sens_recv.at[t - 1], (grp, at(t))).wait_recv()

    s1, s2, s3, both = "s1", "s2", "s3", (0, 1)
    does = {
        s1: stage1, s2: stage2, s3: stage3, "core": lambda kk, c: to_peer(kk, c).start(), "meet": meet, "late": late,
    }
    pair = lambda name, *units: [(name, u, c) for u in units for c in both]
    after = {
        0: [("meet",)],
        5: pair("core", 1),
        9: pair("core", 2) + pair(s1, 2),
        11: pair(s1, 0, 1),
        13: pair("core", 5) + pair(s1, 3) + pair(s2, 2),
        15: pair(s1, 4) + pair(s2, 0),
        17: pair("core", 4) + pair(s2, 1, 3) + pair(s3, 2),
        19: pair(s1, 5) + pair(s2, 4) + pair(s3, 0),
        20: [("core", 3, 0)] + pair(s3, 1, 3),
        21: [("core", 3, 1)],
        22: [(s1, 6, 0)] + pair(s2, 5),
        23: [(s1, 6, 1)] + pair(s3, 4) + pair(s2, 6) + pair(s3, 5, 6),
    }
    after.setdefault(9, []).append(("late",))
    prepare(0)
    block(-1)
    for n in range(4 * STEPS):
        if n % 2 == 1 and n + 1 < 4 * STEPS:
            if n % 4 == 3:
                scoped(f"sens_wait_{n}", arrived, (n + 1) // 2)
            prepare((n + 1) // 2)
        block(n)
        for name, *args in after.get(n, ()):
            scoped("_".join([name, *map(str, args)]), does[name], *args)

    def landed(q, away, h):
        for c in both:
            slot = rcv.at[q, away, h, c]
            copy(slot, slot, f_send.at[0, 0, 0], f_recv.at[q, away, h, c], (other, blk)).wait_recv()

    def total(slots, h, c):
        base = None
        for q, away in slots:
            term = rcv[q, away, h, c].astype(F32)
            base = term if base is None else base + term
        return base

    def gather():
        pl.when(core == 1)(lambda: landed(0, 0, 0))
        for h in both:
            landed(0, 1, h)
            landed(2, 0, h)
            landed(2, 1, h)

            @pl.when(core == 0)
            def _(h=h):
                landed(3, 0, h)
                landed(3, 1, h)

            landed(1, 0, h)
            landed(1, 1, h)

    scoped("gather", gather)
    for h in both:
        for c in both:
            part = total([(q, away) for q in range(3) for away in both], h, c)
            far_part = total([(3, 0), (3, 1)], h, c)
            first = h * half + c * chunk
            out[:, first : first + chunk] = jnp.where(core == 0, part + far_part, part)

    for o in range(1, STEPS):
        copy(sens_in.at[0], sens_in.at[o], sens_send.at[o - 1], sens_recv.at[o - 1], (grp, at(-o))).wait_send()
    for kk in range(1, STEPS):
        for c in both:
            to_peer(kk, c).wait_send()
    for sent in started:
        sent.wait_send()
    for u in range(7):
        for c in both:
            final(u, c, 1).wait_send()
            if u in holder:
                pl.when(core != holder[u])(lambda u=u, c=c: final(u, c, 0).wait_send())
            else:
                final(u, c, 0).wait_send()


def solution(mesh):
    groups, blocks = mesh.shape["grp"], mesh.shape["blk"]

    def step(sensors, sources, weights, probes):
        (columns, probe), count = (sensors.shape[1], probes.shape[1]), probes.shape[0]
        rows, half, chunk = probe // groups, columns // 2, columns // 4
        dma = pltpu.SemaphoreType.DMA
        return pl.pallas_call(
            functools.partial(kernel, groups, blocks),
            out_shape=jax.ShapeDtypeStruct((rows, columns), F32),
            in_specs=[pl.BlockSpec(memory_space=pltpu.HBM)] * 4,
            out_specs=pl.BlockSpec(memory_space=pltpu.VMEM),
            scratch_shapes=[
                pltpu.VMEM((3, columns), F32),
                pltpu.VMEM((count, probe), BF),
                pltpu.VMEM((3, count), BF),
                pltpu.VMEM((count // 128, 128), BF),
                pltpu.VMEM((probe, count), BF),
                pltpu.VMEM((count, 128), BF),
                pltpu.VMEM((3, count if ON_MXU < chunk else 16, 128), BF),
                pltpu.VMEM((2, 128, half), BF),
                pltpu.VMEM((2, 8, half), F32),
                pltpu.VMEM((count, chunk), BF),
                pltpu.VMEM((count, chunk), BF),
                pltpu.VMEM((STEPS, 8, 3 * columns // 8), F32),
                pltpu.VMEM((12, 2, groups, rows, chunk), BF),
                pltpu.VMEM((5, 2, groups, rows, chunk), BF),
                pltpu.VMEM((7, 2, rows, chunk), BF),
                pltpu.VMEM((7, 2, rows, chunk), BF),
                pltpu.VMEM((7, 2, 2, rows, chunk), BF),
                pltpu.VMEM((7, 2, 2, rows, chunk), BF),
                pltpu.VMEM((4, 2, 2, 2, rows, chunk), BF),
                dma((4,)),
                pltpu.SemaphoreType.REGULAR((5,)),
                dma((5,)),
                dma((5,)),
                dma((5, 2)),
                dma((5, 2)),
            ]
            + [dma((7, 2))] * 8
            + [dma((7, 2, 2)), dma((4, 2, 2, 2))],
            compiler_params=pltpu.CompilerParams(collective_id=0, has_side_effects=True, vmem_limit_bytes=63500000),
        )(sensors, sources, weights.reshape(-1, 128), probes)

    in_specs = (P(None, "blk"), P(None, ("grp", "blk")), P(("grp", "blk")), P(("grp", "blk"), None))
    return jax.shard_map(step, mesh=mesh, in_specs=in_specs, out_specs=P("grp", "blk"), check_vma=False)
```

```python
import functools
import math

import jax
import jax.numpy as jnp
from jax import lax
from jax.experimental import pallas as pl
from jax.experimental.pallas import tpu as pltpu
from jax.sharding import PartitionSpec as P

STEPS = 6
EPS = 0.0025
BF, F32 = jnp.bfloat16, jnp.float32
MESH = pl.DeviceIdType.MESH

ORDER = ((0, 0, 1, 1, 2, 2, 5, 5, 4, 4, 3, 3), (1, 1, 2, 2, 6, 6, 5, 5, 4, 4, 3, 3))
NEEDED = (1, 2, 5, 4, 3)
TILE = 256
ON_MXU = 256


def pieces(v):
    hi = v.astype(BF).astype(F32)
    mid = (v - hi).astype(BF).astype(F32)
    return [hi, mid, v - hi - mid]


def squared(v):
    return v[0:1] * v[0:1] + v[1:2] * v[1:2] + v[2:3] * v[2:3]


def kernel(
    groups, blocks, sens, src, wgt, prb, out, own_sens, prb_in, src_in, wgt_in, prb_t, lhs, lanes, rhs, rows_of, ker_a, ker_b, sens_in, work,
    inbox, buf_a, buf_b, buf_c, buf_d, rcv, load, ready, sens_send, sens_recv, core_send, core_recv, a_send, a_recv, b_send, b_recv,
    c_send, c_recv, d_send, d_recv, f_send, f_recv,
):
    sources, sensors = src.shape[1], sens.shape[1]
    half, chunk = sensors // 2, sensors // 4
    nx = groups // 2
    grp, blk = lax.axis_index("grp"), lax.axis_index("blk")
    x, yh = grp // 2, grp % 2
    core = blk % 2
    other = grp + 1 - 2 * yh
    x_next = ((x + 1) % nx) * 2 + yh
    x_prev = ((x + nx - 1) % nx) * 2 + yh
    peer = blk + 1 - 2 * core

    def at(offset):
        return (blk + offset + blocks) % blocks

    def by_core(a, b):
        return a if a == b else jnp.where(core == 0, a, b)

    def signal(semaphore, device):
        pl.semaphore_signal(semaphore, inc=1, device_id=device, device_id_type=MESH)

    def copy(source, target, send, recv, device):
        return pltpu.make_async_remote_copy(source, target, send, recv, device_id=device, device_id_type=MESH)

    started = []

    def send(*args):
        started.append(copy(*args))
        started[-1].start()

    barrier = pltpu.get_barrier_semaphore()
    for o in range(1, STEPS):
        signal(barrier, (grp, at(-o)))
        pl.when(blk + o < blocks)(lambda o=o: signal(barrier, (grp, at(o))))
    for o in range(STEPS):
        signal(barrier, (other, at(-o)))
    for row in (x_next, x_prev):
        signal(barrier, (row, blk))
    expected = 3 * STEPS - jnp.maximum(STEPS - 1 - blk, 0)

    loads = [
        pltpu.make_async_copy(ref, target, load.at[i])
        for i, (ref, target) in enumerate(((src, src_in), (sens, own_sens), (wgt, wgt_in), (prb, prb_in)))
    ]
    for step in loads:
        step.start()
    rhs[...] = jnp.zeros_like(rhs)

    loads[0].wait()
    place = src_in[...].astype(F32)
    rows = [-2.0 * place] * 3 + [jnp.ones((3, sources), F32)] + pieces(squared(place)) + [jnp.zeros((113, sources), F32)]
    lhs[...] = jnp.transpose(jnp.concatenate(rows, axis=0)).astype(BF)
    if ON_MXU < chunk:
        row, column = (lax.broadcasted_iota(jnp.int32, (128, 384), d) for d in range(2))
        spread = jnp.where(row == column // 128, -0.5, 0.0).astype(BF)
        copies = jnp.dot(lhs[...], spread, preferred_element_type=F32).astype(BF)
        for i in range(3):
            lanes[i] = copies[:, i * 128 : (i + 1) * 128]
    @pl.when(blk > blocks - STEPS)
    def _():
        pl.semaphore_wait(barrier, expected)
        for o in range(1, STEPS):
            pl.when(blk + o >= blocks)(lambda o=o: signal(ready.at[o - 1], (grp, at(o))))

    loads[1].wait()
    width = sensors // 8
    for r in range(8):
        span = slice(r * width, (r + 1) * width)
        sens_in[0, r : r + 1] = jnp.concatenate([own_sens[i : i + 1, span] for i in range(3)], axis=1)
    loads[2].wait()
    scale = 1.0 / math.sqrt(STEPS * sources * groups)
    weight = wgt_in[...].astype(F32) * scale
    weight = jnp.concatenate([weight[i : i + 1] for i in range(weight.shape[0])], axis=1)
    loads[3].wait()
    prb_t[...] = (jnp.transpose(prb_in[...]).astype(F32) * weight).astype(BF)

    def turn(hs):
        return by_core(ORDER[0][hs], ORDER[1][hs]), hs % 2

    def slot_of(hs):
        kk0, kk1 = ORDER[0][hs], ORDER[1][hs]
        j = hs % 2
        return by_core(j if kk0 == 0 else 2 * kk0 + 1 - j, j if kk1 == 6 else 2 * kk1 + 1 - j)

    def prepare(hs):
        kk, j = turn(hs)
        packed = sens_in[kk - core]
        packed = jnp.where(core == j, packed[4:8], packed[0:4])
        where = jnp.concatenate(
            [jnp.concatenate([packed[r : r + 1, i * width : (i + 1) * width] for r in range(4)], axis=1) for i in range(3)], axis=0
        )
        parts = pieces(where)
        rows = parts + pieces(squared(where) + EPS) + [jnp.ones((3, half), F32), jnp.zeros((1, half), F32)]
        rhs[hs % 2, 0:16] = jnp.concatenate(rows, axis=0).astype(BF)
        rows_of[hs % 2] = jnp.concatenate([parts[0], where - parts[0], jnp.zeros((2, half), F32)], axis=0)

    def evaluate(n, k):
        ker, hs, first = (ker_a, ker_b)[n % 2], n // 2, (n % 2) * chunk
        span = pl.ds(k * TILE, TILE)
        dist = jnp.dot(lhs[span], rhs[hs % 2, :, pl.ds(first, ON_MXU)], preferred_element_type=F32)
        ker[span, 0:ON_MXU] = lax.rsqrt(dist).astype(BF)
        width = chunk - ON_MXU
        if width == 0:
            return
        near = [
            jnp.broadcast_to(rows_of[hs % 2, i : i + 1, pl.ds(first + ON_MXU, width)], (16, width)).astype(BF) for i in range(6)
        ]
        for r in range(k * TILE, (k + 1) * TILE, 16):
            total = None
            for i in range(3):
                delta = jnp.concatenate([lanes[i, r : r + 16]] * (width // 128), axis=1) - near[i] - near[3 + i]
                total = delta * delta if total is None else total + delta * delta
            ker[r : r + 16, ON_MXU:chunk] = lax.rsqrt(total + jnp.asarray(EPS, BF))

    def block(n):
        part = None
        for k in range(sources // TILE):
            if n + 1 < 4 * STEPS:
                evaluate(n + 1, k)
            if n >= 0:
                span = pl.ds(k * TILE, TILE)
                term = jnp.dot(prb_t[:, span], (ker_a, ker_b)[n % 2][span], preferred_element_type=F32)
                part = term if part is None else part + term
        if n >= 0:
            part = part.astype(BF).reshape(groups, part.shape[0] // groups, chunk)
            work[slot_of(n // 2), n % 2] = part

    def unit_kk(u):
        return 6 * core if u < 2 else (1, 2, 5, 4, 3)[u - 2]

    def unit_at(u):
        return u if u < 2 else 2 * unit_kk(u)

    def unit_half(u):
        return core if u > 0 else 1 - core

    far, fore, back = (x + 2) % nx * 2, (x + 1) % nx * 2, (x + nx - 1) % nx * 2

    def to_peer(kk, c):
        s = kk - 1
        return copy(work.at[2 * kk + 1, c], inbox.at[s, c], core_send.at[s, c], core_recv.at[s, c], (grp, peer))

    def stage1(u, c):
        w = unit_at(u)
        if u >= 2:
            kk = unit_kk(u)
            to_peer(kk, c).wait_recv()
            work[w, c] = (work[w, c].astype(F32) + inbox[kk - 1, c].astype(F32)).astype(BF)
        send(work.at[w, c, far], buf_a.at[u, c], a_send.at[u, c], a_recv.at[u, c], (x_next, blk))
        send(work.at[w, c, far + 1], buf_b.at[u, c], b_send.at[u, c], b_recv.at[u, c], (x_prev, blk))

    def stage2(u, c):
        w = unit_at(u)
        copy(buf_a.at[u, c], buf_a.at[u, c], a_send.at[u, c], a_recv.at[u, c], (x_prev, blk)).wait_recv()
        work[w, c, fore] = (work[w, c, fore].astype(F32) + buf_a[u, c].astype(F32)).astype(BF)
        send(work.at[w, c, pl.ds(fore, 2)], buf_c.at[u, c], c_send.at[u, c], c_recv.at[u, c], (x_next, blk))
        copy(buf_b.at[u, c], buf_b.at[u, c], b_send.at[u, c], b_recv.at[u, c], (x_next, blk)).wait_recv()
        work[w, c, back + 1] = (work[w, c, back + 1].astype(F32) + buf_b[u, c].astype(F32)).astype(BF)
        send(work.at[w, c, pl.ds(back, 2)], buf_d.at[u, c], d_send.at[u, c], d_recv.at[u, c], (x_prev, blk))

    def final(u, c, away):
        w, kk, h = unit_at(u), unit_kk(u), unit_half(u)
        row = grp if away == 0 else other
        q = kk // 2
        return copy(work.at[w, c, row], rcv.at[q, away, h, c], f_send.at[u, c, away], f_recv.at[q, away, h, c], (row, at(kk - core)))

    holder = {0: 0, 1: 0, 2: 1}

    def stage3(u, c):
        w, h = unit_at(u), unit_half(u)
        copy(buf_c.at[u, c], buf_c.at[u, c], c_send.at[u, c], c_recv.at[u, c], (x_prev, blk)).wait_recv()
        copy(buf_d.at[u, c], buf_d.at[u, c], d_send.at[u, c], d_recv.at[u, c], (x_next, blk)).wait_recv()
        own = pl.ds(x * 2, 2)
        work[w, c, own] = (work[w, c, own].astype(F32) + buf_c[u, c].astype(F32) + buf_d[u, c].astype(F32)).astype(BF)
        final(u, c, 1).start()
        if u in holder:

            @pl.when(core == holder[u])
            def _():
                rcv[0, 0, h, c] = work[w, c, grp]

            @pl.when(core != holder[u])
            def _():
                final(u, c, 0).start()
        else:
            final(u, c, 0).start()

    def sensors_to(o):
        copy(sens_in.at[0], sens_in.at[o], sens_send.at[o - 1], sens_recv.at[o - 1], (grp, at(-o))).start()

    def sensors_late(o):
        pl.semaphore_wait(ready.at[o - 1], 1)
        sensors_to(o)

    def meet():
        with jax.named_scope("barrier_wait"):
            pl.when(blk <= blocks - STEPS)(lambda: pl.semaphore_wait(barrier, expected))
        for o in NEEDED:
            pl.when(blk >= o)(lambda o=o: sensors_to(o))

    def scoped(name, action, *args):
        with jax.named_scope(name):
            action(*args)

    def late():
        for o in NEEDED:
            pl.when(blk < o)(functools.partial(sensors_late, o))

    def arrived(hs):
        t = turn(hs)[0] - core
        copy(sens_in.at[0], sens_in.at[t], sens_send.at[t - 1], sens_recv.at[t - 1], (grp, at(t))).wait_recv()

    s1, s2, s3, both = "s1", "s2", "s3", (0, 1)
    does = {
        s1: stage1, s2: stage2, s3: stage3, "core": lambda kk, c: to_peer(kk, c).start(), "meet": meet, "late": late,
    }
    pair = lambda name, *units: [(name, u, c) for u in units for c in both]
    after = {
        0: [("meet",)],
        5: pair("core", 1),
        9: pair("core", 2) + pair(s1, 2),
        11: pair(s1, 0, 1),
        13: pair("core", 5) + pair(s1, 3) + pair(s2, 2),
        15: pair(s1, 4) + pair(s2, 0),
        17: pair("core", 4) + pair(s2, 1, 3) + pair(s3, 2),
        19: pair(s1, 5) + pair(s2, 4) + pair(s3, 0),
        20: [("core", 3, 0)] + pair(s3, 1, 3),
        21: [("core", 3, 1)],
        22: [(s1, 6, 0)] + pair(s2, 5),
        23: [(s1, 6, 1)] + pair(s3, 4) + pair(s2, 6) + pair(s3, 5, 6),
    }
    after.setdefault(7, []).append(("late",))
    prepare(0)
    block(-1)
    for n in range(4 * STEPS):
        if n % 2 == 1 and n + 1 < 4 * STEPS:
            if n % 4 == 3:
                scoped(f"sens_wait_{n}", arrived, (n + 1) // 2)
            prepare((n + 1) // 2)
        block(n)
        for name, *args in after.get(n, ()):
            scoped("_".join([name, *map(str, args)]), does[name], *args)

    def landed(q, away, h):
        for c in both:
            slot = rcv.at[q, away, h, c]
            copy(slot, slot, f_send.at[0, 0, 0], f_recv.at[q, away, h, c], (other, blk)).wait_recv()

    def total(slots, h, c):
        base = None
        for q, away in slots:
            term = rcv[q, away, h, c].astype(F32)
            base = term if base is None else base + term
        return base

    def gather():
        pl.when(core == 1)(lambda: landed(0, 0, 0))
        for h in both:
            landed(0, 1, h)
            landed(2, 0, h)
            landed(2, 1, h)

            @pl.when(core == 0)
            def _(h=h):
                landed(3, 0, h)
                landed(3, 1, h)

            landed(1, 0, h)
            landed(1, 1, h)

    def finish(*units):
        for u in units:
            for c in both:
                final(u, c, 1).wait_send()
                if u in holder:
                    pl.when(core != holder[u])(lambda u=u, c=c: final(u, c, 0).wait_send())
                else:
                    final(u, c, 0).wait_send()

    for o in range(1, STEPS):
        copy(sens_in.at[0], sens_in.at[o], sens_send.at[o - 1], sens_recv.at[o - 1], (grp, at(-o))).wait_send()
    for kk in range(1, STEPS):
        for c in both:
            to_peer(kk, c).wait_send()
    for sent in started:
        sent.wait_send()
    finish(0, 1, 2, 3, 4)
    scoped("gather", gather)
    for h in both:
        for c in both:
            part = total([(q, away) for q in range(3) for away in both], h, c)
            far_part = total([(3, 0), (3, 1)], h, c)
            first = h * half + c * chunk
            out[:, first : first + chunk] = jnp.where(core == 0, part + far_part, part)

    finish(5, 6)


def solution(mesh):
    groups, blocks = mesh.shape["grp"], mesh.shape["blk"]

    def step(sensors, sources, weights, probes):
        (columns, probe), count = (sensors.shape[1], probes.shape[1]), probes.shape[0]
        rows, half, chunk = probe // groups, columns // 2, columns // 4
        dma = pltpu.SemaphoreType.DMA
        return pl.pallas_call(
            functools.partial(kernel, groups, blocks),
            out_shape=jax.ShapeDtypeStruct((rows, columns), F32),
            in_specs=[pl.BlockSpec(memory_space=pltpu.HBM)] * 4,
            out_specs=pl.BlockSpec(memory_space=pltpu.VMEM),
            scratch_shapes=[
                pltpu.VMEM((3, columns), F32),
                pltpu.VMEM((count, probe), BF),
                pltpu.VMEM((3, count), BF),
                pltpu.VMEM((count // 128, 128), BF),
                pltpu.VMEM((probe, count), BF),
                pltpu.VMEM((count, 128), BF),
                pltpu.VMEM((3, count if ON_MXU < chunk else 16, 128), BF),
                pltpu.VMEM((2, 128, half), BF),
                pltpu.VMEM((2, 8, half), F32),
                pltpu.VMEM((count, chunk), BF),
                pltpu.VMEM((count, chunk), BF),
                pltpu.VMEM((STEPS, 8, 3 * columns // 8), F32),
                pltpu.VMEM((12, 2, groups, rows, chunk), BF),
                pltpu.VMEM((5, 2, groups, rows, chunk), BF),
                pltpu.VMEM((7, 2, rows, chunk), BF),
                pltpu.VMEM((7, 2, rows, chunk), BF),
                pltpu.VMEM((7, 2, 2, rows, chunk), BF),
                pltpu.VMEM((7, 2, 2, rows, chunk), BF),
                pltpu.VMEM((4, 2, 2, 2, rows, chunk), BF),
                dma((4,)),
                pltpu.SemaphoreType.REGULAR((5,)),
                dma((5,)),
                dma((5,)),
                dma((5, 2)),
                dma((5, 2)),
            ]
            + [dma((7, 2))] * 8
            + [dma((7, 2, 2)), dma((4, 2, 2, 2))],
            compiler_params=pltpu.CompilerParams(collective_id=0, has_side_effects=True, vmem_limit_bytes=63500000),
        )(sensors, sources, weights.reshape(-1, 128), probes)

    in_specs = (P(None, "blk"), P(None, ("grp", "blk")), P(("grp", "blk")), P(("grp", "blk"), None))
    return jax.shard_map(step, mesh=mesh, in_specs=in_specs, out_specs=P("grp", "blk"), check_vma=False)
```
